256 devices in a mesh: slab: 8 (over y, core), bl: 32 (over z, x).
Axes of the slice: x: 4, y: 4, z: 8, core: 2. Of those that a mesh axis runs over, the one named last changes fastest.
Arguments:
- model_image: float32 [2, 8192, 8192], P(None, 'slab', 'bl'), may hold values from -6 to 6
- vis_coords: float32 [4096, 2, 128], P(('slab', 'bl')), may hold values from 0 to 32
- vis_observed: float32 [4096, 2, 128], P(('slab', 'bl')), may hold values from -6 to 6
- tile_slot: int32 [4096], P(('slab', 'bl')), may hold values from 0 to 255
- tile_group: int32 [4096, 1], P(('slab', 'bl')), may hold values from 0 to 31; in each aligned block of 16 rows (0 to 15, 16 to 31, ...) at most 2 rows name the same one
- w_plane: int32 [4096], P(('slab', 'bl')), may hold values from 0 to 7
- vis_count: int32 [4096], P(('slab', 'bl')), may hold values from 16 to 128, as said below
Outputs:
- residual_image: float32 [2, 8192, 8192], P(None, 'slab', 'bl')
- residual_vis: float32 [4096, 2, 128], P(('slab', 'bl'))
The draws below stay inside these ranges and needn't reach their ends.
Inputs may be any that keep to these rules, and one draw needn't show every extreme that they name: `tile_group`: among the 16 subgrids of one device, at most 2 name the same group. `vis_count`: some subgrid holds exactly 128 visibilities.
All inputs are finite; a program needn't handle non-finite values.
Results may differ from the reference program's by a relative error of at most 0.0003.
Values sent between devices are 32-bit elements; how exact they have to be, the bound alone decides.
A program may use at most 128 MiB of HBM per device.

```python
import math
import jax
import jax.numpy as jnp
import numpy as np
from jax import lax

N = 8192
SUB = 32
NW = 8
VPS = 128
SG_DEV = 16
CAP = 2
NSG = 4096
NTILE = 256
TCOLS = 1
N_BL = 32


def draw_vis_count(key, part):
    counts = jax.random.randint(jax.random.fold_in(key, 11), (NSG,), VPS // 8, VPS + 1, dtype=jnp.int32)
    return counts.at[0].set(VPS)


def with_ends(array, rng, smallest, largest):
    spot = [jax.random.randint(jax.random.fold_in(rng, axis), (), 0, length) for axis, length in enumerate(array.shape)]
    widest = array.shape.index(max(array.shape))
    neighbour = spot[:widest] + [(spot[widest] + 1) % array.shape[widest]] + spot[widest + 1:]
    return array.at[tuple(spot)].set(smallest).at[tuple(neighbour)].set(largest)


def shard_levels(rng, extent, shards, smallest, top_value):
    level, own = 1.0, jax.random.fold_in(rng, 6)
    for axis_at, shards_of in shards:
        steps = jnp.exp(jax.random.uniform(jax.random.fold_in(own, axis_at), (shards_of,), jnp.float32, smallest / len(shards), top_value / len(shards)))
        level = level * jnp.repeat(steps, extent[axis_at] // shards_of).reshape([-1 if axis == axis_at else 1 for axis in range(len(extent))])
    return level


def assign_block(key, own, number, rows, amount, top, bound, lean):
    sequence = jax.random.permutation(key, amount)
    heavy_load, usual = shares(amount, rows * top, bound, lean, True), shares(amount, rows * top, bound, lean, False)
    places = jnp.arange(amount)

    def named(lengths, offset_by):
        used = int((lengths > 0).sum())
        fixed = max(1, used // 4)
        passed = fixed + (places - fixed + offset_by * (used - fixed)) % max(1, amount - fixed)
        return jnp.zeros((amount,), jnp.int32).at[sequence[jnp.where(places < fixed, places, passed)]].set(jnp.asarray(lengths, jnp.int32))

    lengths = jnp.where(number % 4 == 0, named(heavy_load, number // 4), named(usual, number - number // 4 - 1))
    mixed = jax.random.permutation(jax.random.fold_in(own, 3), amount)
    giver, receiver = mixed[0:amount // 2 * 2:2], mixed[1:amount // 2 * 2:2]
    margin = jnp.minimum(lengths[giver] - 1, bound - lengths[receiver]) // 2
    margin = jnp.where((giver == sequence[0]) | (receiver == sequence[0]) | (lengths[receiver] == 0), 0, jnp.maximum(margin, 0))
    passed = jax.random.randint(jax.random.fold_in(own, 4), (amount // 2,), 0, 1 << 20) % (margin + 1)
    lengths = lengths.at[giver].add(-passed).at[receiver].add(passed)
    labels = jnp.searchsorted(jnp.cumsum(lengths), jnp.arange(rows * top), side="right").astype(jnp.int32)
    table = labels.reshape(top, rows).T
    table = table[jax.random.permutation(jax.random.fold_in(own, 1), rows)]
    offset_by = jax.random.randint(jax.random.fold_in(own, 2), (rows, 1), 0, top)
    return jnp.take_along_axis(table, (jnp.arange(top)[None, :] + offset_by) % top, axis=1)


def shares(number_of, total, most, lean, full):
    weights = [(1 << 20) // math.isqrt(standing ** lean) + 1 for standing in range(1, number_of + 1)]
    largest = most if full else min(most, max(-(-total // number_of), total * weights[0] // sum(weights)))
    least = 1 if total - largest >= number_of - 1 else 0
    given, spare = [largest] + [least] * (number_of - 1), total - largest - least * (number_of - 1)
    while spare > 0:
        movable = [i for i in range(1, number_of) if given[i] < largest] or [i for i in range(1, number_of) if given[i] < most]
        pool, left = sum([weights[i] for i in movable]), spare
        for i in movable:
            addition = min(most - given[i], max(1, left * weights[i] // pool), spare)
            given[i] = given[i] + addition
            spare = spare - addition
    return np.array(given)


def normal_values(own_key, dims, deviation, reach, cuts=(), held_as=jnp.bfloat16):
    array = jax.random.normal(own_key, dims, jnp.float32) * deviation
    if len(cuts) > 0:
        array = shard_levels(own_key, dims, cuts, -0.22, 0.18) * array
    return jnp.clip(array, min=-reach, max=reach).astype(held_as)


def setup_inputs(seed: int = 0) -> dict:
    seeds = jax.random.split(jax.random.key(seed), 8)
    model_image = normal_values(seeds[0], (2, N, N), 1.0, 6.0, ((1, 8), (2, 32)), jnp.float32)
    vis_coords = jnp.clip(32.0 * jax.random.uniform(seeds[1], (NSG, 2, VPS), jnp.float32) ** shard_levels(seeds[1], (NSG, 2, VPS), ((0, 256),), -0.2, 0.2), 0.0, 32.0)
    vis_observed = normal_values(seeds[2], (NSG, 2, VPS), 1.0, 6.0, ((0, 256),), jnp.float32)
    tile_slot = with_ends(jax.random.randint(seeds[3], (NSG,), 0, NTILE * TCOLS), jax.random.fold_in(seeds[3], 1), 0, (NTILE * TCOLS) - 1).astype(jnp.int32)
    tile_group_keys = jax.random.split(jax.random.fold_in(seeds[4], 1), NSG // SG_DEV)
    tile_group_turns = jax.random.permutation(jax.random.fold_in(seeds[4], 3), NSG // SG_DEV)
    tile_group = jax.vmap(lambda own, number: assign_block(jax.random.fold_in(seeds[4], 2), own, number, SG_DEV, N_BL, 1, CAP, 2))(tile_group_keys, tile_group_turns).reshape((NSG, 1))
    w_plane = with_ends(jax.random.randint(seeds[5], (NSG,), 0, NW), jax.random.fold_in(seeds[5], 1), 0, NW - 1).astype(jnp.int32)
    vis_count = draw_vis_count(jax.random.fold_in(seeds[7], 71), 0)
    return {"model_image": model_image, "vis_coords": vis_coords, "vis_observed": vis_observed, "tile_slot": tile_slot, "tile_group": tile_group, "w_plane": w_plane, "vis_count": vis_count}


w_step = 0.1


def complex_einsum(form, left, right):
    product = lambda first, second: jnp.einsum(form, first, second, precision=lax.Precision.HIGHEST)
    return (product(left[0], right[0]) - product(left[1], right[1]),
            product(left[0], right[1]) + product(left[1], right[0]))


def complex_mul(left, right):
    return (left[0] * right[0] - left[1] * right[1], left[0] * right[1] + left[1] * right[0])


def subgrid_pass(tile_real, tile_imag, coords, observed, planes, counts):
    width = tile_real.shape[-1]
    half = width // 2
    slots = coords.shape[-1]
    index = jnp.arange(width, dtype=jnp.int32)
    offsets = (index - half).astype(jnp.float32)
    turns = (index[:, None] * (index[None, :] - half)) % width
    angle = (2.0 * math.pi / width) * turns.astype(jnp.float32)
    forward_d = (jnp.cos(angle), jnp.sin(angle))
    backward_d = (forward_d[0], -forward_d[1])
    scale_sub = 1.0 / (width * width)
    halfway = complex_einsum('il,kij->klj', forward_d, (tile_real, tile_imag))
    image_sub = complex_einsum('klj,jm->klm', halfway, forward_d)
    image_sub = (image_sub[0] * scale_sub, image_sub[1] * scale_sub)
    radius = (offsets[:, None] ** 2 + offsets[None, :] ** 2) / (half * half)
    phase = -w_step * planes.astype(jnp.float32)[:, None, None] * radius[None]
    screen = (jnp.cos(phase), jnp.sin(phase))
    weighted = complex_mul(screen, image_sub)
    along_a = (-2.0 * math.pi / width) * coords[:, 0, :][:, None, :] * offsets[None, :, None]
    along_b = (-2.0 * math.pi / width) * coords[:, 1, :][:, None, :] * offsets[None, :, None]
    phase_a = (jnp.cos(along_a), jnp.sin(along_a))
    phase_b = (jnp.cos(along_b), jnp.sin(along_b))
    partial_rows = complex_einsum('klm,kmj->klj', weighted, phase_b)
    terms = complex_mul(phase_a, partial_rows)
    predicted = (jnp.sum(terms[0], axis=1), jnp.sum(terms[1], axis=1))
    live = (jnp.arange(slots, dtype=jnp.int32)[None, :] < counts[:, None]).astype(jnp.float32)
    resid_real = (observed[:, 0, :] - predicted[0]) * live
    resid_imag = (observed[:, 1, :] - predicted[1]) * live
    spread = complex_mul((phase_a[0], -phase_a[1]), (resid_real[:, None, :], resid_imag[:, None, :]))
    collected = complex_einsum('klj,kmj->klm', spread, (phase_b[0], -phase_b[1]))
    unscreened = complex_mul((screen[0], -screen[1]), collected)
    middle = complex_einsum('il,klm->kim', backward_d, unscreened)
    tile_out = complex_einsum('kim,jm->kij', middle, backward_d)
    return (jnp.stack([resid_real, resid_imag], axis=1),
            jnp.stack([tile_out[0] * scale_sub, tile_out[1] * scale_sub], axis=1))


def reference(model_image, vis_coords, vis_observed, tile_slot, tile_group, w_plane, vis_count):
    image = lax.complex(model_image[0], model_image[1])
    grid = jnp.fft.fft2(image) / N
    tiles = grid.reshape(NTILE, SUB, NTILE, SUB).transpose(0, 2, 1, 3).reshape(NTILE * NTILE, SUB, SUB)
    index = jnp.arange(NSG, dtype=jnp.int32)
    band = index // (SG_DEV * N_BL)
    column = (band * N_BL + tile_group[:, 0]) * TCOLS + tile_slot // NTILE
    tile_id = ((tile_slot % NTILE) * NTILE + column).astype(jnp.int32)
    blocks = NSG // SG_DEV

    def one_block(pieces):
        block_ids, block_coords, block_obs, block_planes, block_counts = pieces
        chosen = tiles[block_ids]
        return subgrid_pass(jnp.real(chosen), jnp.imag(chosen), block_coords, block_obs, block_planes, block_counts)

    resid_vis, contrib = lax.map(one_block, (
        tile_id.reshape(blocks, SG_DEV),
        vis_coords.reshape(blocks, SG_DEV, 2, VPS),
        vis_observed.reshape(blocks, SG_DEV, 2, VPS),
        w_plane.reshape(blocks, SG_DEV),
        vis_count.reshape(blocks, SG_DEV)))
    resid_vis = resid_vis.reshape(NSG, 2, VPS)
    contrib = contrib.reshape(NSG, 2 * SUB * SUB)
    summed = jax.ops.segment_sum(contrib, tile_id, num_segments=NTILE * NTILE)
    resid_grid = summed.reshape(NTILE, NTILE, 2, SUB, SUB).transpose(2, 0, 3, 1, 4).reshape(2, N, N)
    back = jnp.fft.ifft2(lax.complex(resid_grid[0], resid_grid[1])) * N
    resid_image = jnp.stack([jnp.real(back), jnp.imag(back)]).astype(jnp.float32)
    return resid_image, resid_vis
```

```python
import functools
import math

import jax
import jax.numpy as jnp
import numpy as np
from jax import lax
from jax.experimental import pallas as pl
from jax.experimental.pallas import tpu as pltpu
from jax.sharding import Mesh
from jax.sharding import PartitionSpec as P

N = 8192
SUB = 32
BL = ("bl_0", "bl_1")
SLAB_BL = ("slab", "bl_0", "bl_1")
PLANE = ("slab", "bl_1")
W_STEP = 0.1
F32 = jnp.float32
BF16 = jnp.bfloat16
HIGHEST = lax.Precision.HIGHEST
MESH = pl.DeviceIdType.MESH
ANY = pl.BlockSpec(memory_space=pl.ANY)
DMA = pltpu.SemaphoreType.DMA
VMEM_LIMIT = 62 * 1024 * 1024


def unit(numerator, modulus):
    angle = 2.0 * np.pi * (numerator % modulus) / modulus
    return np.cos(angle), np.sin(angle)


def halves(value):
    high = value.astype(BF16)
    return high, (value - high.astype(F32)).astype(BF16)


def np_halves(value):
    value = np.asarray(value, np.float32)
    high = value.astype(BF16)
    return np.stack([high, (value - high.astype(np.float32)).astype(BF16)])


def row_tables():
    index = np.arange(256)
    cos, sin = unit(np.outer(index, index), 256)
    return np.concatenate([np_halves(cos), np_halves(sin)])


def column_tables():
    a = np.arange(128)[:, None]
    v = np.arange(1024)[None, :]
    cos, sin = unit(a * v, 1024)
    return np.concatenate([np_halves(cos), np_halves(sin)])


def screen_tables():
    b = np.arange(8)[:, None]
    v = np.arange(N)[None, :]
    cos, sin = unit(b * v, N)
    both = np.stack([cos, -sin]).reshape(2, 8, 64, 128)
    return both.transpose(2, 0, 1, 3).astype(np.float32)


def dot(left, right):
    return jnp.dot(left, right, preferred_element_type=F32)


def dot_t(left, right):
    return lax.dot_general(left, right, (((1,), (1,)), ((), ())), preferred_element_type=F32)


def dot3(left, right, product=dot):
    return product(left[0], right[0]) + (product(left[0], right[1]) + product(left[1], right[0]))


def dft4(values, sign):
    (ar, ai), (br, bi), (cr, ci), (dr, di) = values
    pr, pi, mr, mi = ar + cr, ai + ci, ar - cr, ai - ci
    qr, qi, nr, ni = br + dr, bi + di, br - dr, bi - di
    return [
        (pr + qr, pi + qi),
        (mr - sign * ni, mi + sign * nr),
        (pr - qr, pi - qi),
        (mr + sign * ni, mi - sign * nr),
    ]


def turn(value, numerator, modulus, sign):
    cos, sin = math.cos(2 * math.pi * numerator / modulus), sign * math.sin(2 * math.pi * numerator / modulus)
    if numerator % modulus == 0:
        return value
    re, im = value
    return (re * cos - im * sin, re * sin + im * cos)


def dft8(values, sign):
    even, odd = dft4(values[0::2], sign), dft4(values[1::2], sign)
    out = [None] * 8
    for k in range(4):
        tr, ti = turn(odd[k], k, 8, sign)
        out[k] = (even[k][0] + tr, even[k][1] + ti)
        out[k + 4] = (even[k][0] - tr, even[k][1] - ti)
    return out


def butterfly(v_ref, w_ref, rows):
    def tile(step, carry):
        lanes = pl.ds(pl.multiple_of(step * 128, 128), 128)
        mid = []
        for b in range(4):
            column = dft8([(v_ref[s, 0, b, rows, lanes], v_ref[s, 1, b, rows, lanes]) for s in range(8)], -1.0)
            mid.append([turn(column[i0], i0 * b, 32, -1.0) for i0 in range(8)])
        for i0 in range(8):
            done = dft4([mid[b][i0] for b in range(4)], -1.0)
            for i1 in range(4):
                w_ref[i0 + 8 * i1, 0, rows, lanes] = done[i1][0]
                w_ref[i0 + 8 * i1, 1, rows, lanes] = done[i1][1]
        return carry

    lax.fori_loop(0, 2, tile, 0)


def unbutterfly(w_ref, v_ref, rows):
    def tile(step, carry):
        lanes = pl.ds(pl.multiple_of(step * 128, 128), 128)
        mid = []
        for i0 in range(8):
            column = dft4([(w_ref[i0 + 8 * i1, 0, rows, lanes], w_ref[i0 + 8 * i1, 1, rows, lanes]) for i1 in range(4)], 1.0)
            mid.append([turn(column[b], i0 * b, 32, 1.0) for b in range(4)])
        for b in range(4):
            done = dft8([mid[i0][b] for i0 in range(8)], 1.0)
            for s in range(8):
                v_ref[s, 0, b, rows, lanes] = done[s][0]
                v_ref[s, 1, b, rows, lanes] = done[s][1]
        return carry

    lax.fori_loop(0, 2, tile, 0)


def remote(src, dst, send, recv, device):
    return pltpu.make_async_remote_copy(
        src_ref=src, dst_ref=dst, send_sem=send, recv_sem=recv, device_id=device, device_id_type=MESH
    )


def each(count, body):
    def step(at, carry):
        body(at)
        return carry

    lax.fori_loop(1, count, step, 0)


def place_of(peer, z):
    return (peer // 4, z, peer % 4)


def greet(plane, along_z):
    slab, z, x = (lax.axis_index(a) for a in SLAB_BL)
    own = slab * 4 + x
    barrier = pltpu.get_barrier_semaphore()
    if plane:
        each(32, lambda d: pl.semaphore_signal(barrier, inc=1, device_id=place_of((own + d) % 32, z), device_id_type=MESH))
    if along_z:
        each(8, lambda d: pl.semaphore_signal(barrier, inc=1, device_id=(slab, (z + d) % 8, x), device_id_type=MESH))
    pl.semaphore_wait(barrier, 31 * plane + 7 * along_z)
    return slab, z, x, own


def eight(c):
    return pl.ds(8 * c, 8)


def forward_kernel(image_ref, word_ref, a_ref, idx_ref, v_ref, w_ref, zrow_ref, row_ref, local, send1, recv1, send2, recv2, sendz, recvz, sendi, recvi):
    slab, z, x, own = greet(True, True)

    def word_copy(d):
        peer = (z + d) % 8
        return remote(word_ref, zrow_ref.at[z], sendz.at[d], recvz.at[z], (slab, peer, x))

    def slab_copy(c, d):
        peer = (slab + d) % 8
        return remote(image_ref.at[:, :, peer, eight(c)], v_ref.at[slab, :, :, eight(c)], send1.at[c, d], recv1.at[c, slab], (peer, z, x))

    def slab_wait(c, d):
        peer = (slab + d) % 8
        remote(image_ref.at[:, :, peer, eight(c)], v_ref.at[peer, :, :, eight(c)], send1.at[c, d], recv1.at[c, peer], (peer, z, x)).wait_recv()

    def plane_copy(c, d):
        peer = (own + d) % 32
        return remote(w_ref.at[peer, :, eight(c)], a_ref.at[own, :, eight(c)], send2.at[c, d], recv2.at[c, own], place_of(peer, z))

    def plane_wait(c, d):
        peer = (own + d) % 32
        remote(w_ref.at[peer, :, eight(c)], a_ref.at[peer, :, eight(c)], send2.at[c, d], recv2.at[c, peer], place_of(peer, z)).wait_recv()

    def row_copy(d):
        return remote(row_ref, idx_ref.at[own], sendi.at[d], recvi.at[own], place_of((own + d) % 32, z))

    each(8, lambda d: word_copy(d).start())
    mine = pltpu.make_async_copy(image_ref.at[:, :, slab], v_ref.at[slab], local)
    mine.start()
    for c in range(4):
        each(8, lambda d: slab_copy(c, d).start())

    def word_wait(d):
        peer = (z + d) % 8
        remote(word_ref, zrow_ref.at[peer], sendz.at[d], recvz.at[peer], (slab, peer, x)).wait_recv()

    each(8, word_wait)
    zrow_ref[z] = word_ref[...]
    row = zrow_ref[0]
    for at in range(1, 8):
        row = row + zrow_ref[at]
    row_ref[...] = row
    idx_ref[own] = row
    mine.wait()
    for c in range(4):
        each(8, lambda d: slab_wait(c, d))
        if c == 0:
            each(32, lambda d: row_copy(d).start())
        butterfly(v_ref, w_ref, eight(c))
        each(32, lambda d: plane_copy(c, d).start())
        a_ref[own, :, eight(c)] = w_ref[own, :, eight(c)]

    def row_wait(d):
        peer = (own + d) % 32
        remote(row_ref, idx_ref.at[peer], sendi.at[d], recvi.at[peer], place_of(peer, z)).wait_recv()

    each(32, row_wait)
    for c in range(4):
        each(32, lambda d: plane_wait(c, d))
    each(8, lambda d: word_copy(d).wait_send())
    each(32, lambda d: row_copy(d).wait_send())
    for c in range(4):
        each(8, lambda d: slab_copy(c, d).wait_send())
        each(32, lambda d: plane_copy(c, d).wait_send())


def backward_kernel(spot_ref, out_ref, w_ref, v_ref, local, keep, send1, recv1, send2, recv2):
    slab, z, x, own = greet(True, False)

    def plane_copy(c, d):
        peer = (own + d) % 32
        return remote(spot_ref.at[peer, :, eight(c)], w_ref.at[own, :, eight(c)], send1.at[c, d], recv1.at[c, own], place_of(peer, z))

    def plane_wait(c, d):
        peer = (own + d) % 32
        remote(spot_ref.at[peer, :, eight(c)], w_ref.at[peer, :, eight(c)], send1.at[c, d], recv1.at[c, peer], place_of(peer, z)).wait_recv()

    def slab_copy(c, d):
        peer = (slab + d) % 8
        return remote(v_ref.at[peer, :, :, eight(c)], out_ref.at[:, :, slab, eight(c)], send2.at[c, d], recv2.at[c, slab], (peer, z, x))

    def slab_wait(c, d):
        peer = (slab + d) % 8
        remote(v_ref.at[peer, :, :, eight(c)], out_ref.at[:, :, peer, eight(c)], send2.at[c, d], recv2.at[c, peer], (peer, z, x)).wait_recv()

    mine = pltpu.make_async_copy(spot_ref.at[own], w_ref.at[own], local)
    mine.start()
    for c in range(4):
        each(32, lambda d: plane_copy(c, d).start())
    mine.wait()
    kept = []
    for c in range(4):
        each(32, lambda d: plane_wait(c, d))
        unbutterfly(w_ref, v_ref, eight(c))
        each(8, lambda d: slab_copy(c, d).start())
        copy = pltpu.make_async_copy(v_ref.at[slab, :, :, eight(c)], out_ref.at[:, :, slab, eight(c)], keep.at[c])
        copy.start()
        kept.append(copy)
    for c in range(4):
        each(8, lambda d: slab_wait(c, d))
        kept[c].wait()
    for c in range(4):
        each(32, lambda d: plane_copy(c, d).wait_send())
        each(8, lambda d: slab_copy(c, d).wait_send())


def placing(x):
    c0 = lax.broadcasted_iota(jnp.int32, (256, 1024), 0)
    n = lax.broadcasted_iota(jnp.int32, (256, 1024), 1)
    hit = (c0 == 8 * (n & 31) + (n >> 7)) & (((n >> 5) & 3) == x)
    return jnp.where(hit, 1.0, 0.0).astype(BF16)


def spread_screens(w4_ref, w_ref):
    group = lax.broadcasted_iota(jnp.int32, (8, 128), 1) >> 5

    def expand(q, carry):
        for m in range(4):
            mask = group == m
            w_ref[4 * q + m, 0] = jnp.where(mask, w4_ref[q, 0], 0.0)
            w_ref[4 * q + m, 1] = jnp.where(mask, w4_ref[q, 1], 0.0)
        return carry

    lax.fori_loop(0, 64, expand, 0)


def fill_columns(m1_ref, full_ref):
    for h in range(2):
        cos, sin = m1_ref[h], m1_ref[2 + h]
        full_ref[h, 0:128, 0:1024] = cos
        full_ref[h, 0:128, 1024:2048] = -sin
        full_ref[h, 128:256, 0:1024] = sin
        full_ref[h, 128:256, 1024:2048] = cos


def gather_kernel(idx_ref, a_ref, tw_ref, m_ref, m1_ref, w4_ref, phz_ref, out_ref, w_ref, full_ref, high_ref, low_ref, z_ref):
    spread_screens(w4_ref, w_ref)
    fill_columns(m1_ref, full_ref)
    cos, sin = (m_ref[0], m_ref[1]), (m_ref[2], m_ref[3])
    twr = jnp.concatenate([tw_ref[0]] * 2, axis=1)
    twi = jnp.concatenate([tw_ref[1]] * 2, axis=1)
    total = [None] * 4
    for x in range(4):
        ar = a_ref[:, x, 0].reshape(256, 256)
        ai = a_ref[:, x, 1].reshape(256, 256)
        br, bi = halves(ar * twr - ai * twi), halves(ar * twi + ai * twr)
        ur = dot3(cos, br) + dot3(sin, bi)
        ui = dot3(cos, bi) - dot3(sin, br)
        place = placing(x)
        for at, piece in enumerate(halves(ur) + halves(ui)):
            part = dot(piece, place)
            total[at] = part if total[at] is None else total[at] + part
    for b in range(8):
        cut = slice(128 * b, 128 * b + 128)
        rows = pl.ds(b, 256, stride=8)
        for part in range(2):
            high_ref[part, rows, :] = total[2 * part][:, cut]
            low_ref[part, rows, :] = total[2 * part + 1][:, cut]

    def stage(step, carry):
        block, part = step // 4, step % 4
        rows = pl.ds(pl.multiple_of(part * 512, 512), 512)
        lanes = pl.ds(pl.multiple_of(block * 256, 256), 256)
        left = tuple(jnp.concatenate([ref[0, rows, :], ref[1, rows, :]], axis=1).astype(BF16) for ref in (high_ref, low_ref))
        right = (full_ref[0, :, lanes], full_ref[1, :, lanes])
        res = dot3(left, right)
        tus = pl.ds(pl.multiple_of(part * 64, 64), 64)
        z_ref[2 * block, tus] = res[:, 0:128].reshape(64, 8, 128)
        z_ref[2 * block + 1, tus] = res[:, 128:256].reshape(64, 8, 128)
        return carry

    lax.fori_loop(0, 32, stage, 0)

    lane = lax.broadcasted_iota(jnp.int32, (8, 128), 1)
    phr, phi = phz_ref[0:1, :], phz_ref[1:2, :]

    def fold(parts):
        total = jnp.sum(jnp.stack(parts), axis=1)
        total = total + pltpu.roll(total, 64, 1)
        return total + pltpu.roll(total, 32, 1)

    def collect(it, carry):
        both = []
        for half in range(2):
            res, ims = [], []
            for k in range(8):
                word = idx_ref[it % 32, 0, it // 32 * 16 + half * 8 + k]
                tu, tv = word & 255, word >> 8
                t = (tv >> 2) & 7
                zr, zi = z_ref[t, tu], z_ref[8 + t, tu]
                wr, wi = w_ref[tv, 0], w_ref[tv, 1]
                res.append(zr * wr - zi * wi)
                ims.append(zr * wi + zi * wr)
            sr, si = fold(res), fold(ims)
            both += [sr * phr - si * phi, sr * phi + si * phr]
        out = jnp.where(lane < 64, jnp.where(lane < 32, both[0], both[1]), jnp.where(lane < 96, both[2], both[3]))
        out_ref[pl.ds(pl.multiple_of(it * 8, 8), 8), :] = out
        return carry

    lax.fori_loop(0, 256, collect, 0)


def scatter_kernel(idx_ref, c_ref, tw_ref, m_ref, m1_ref, w4_ref, f_ref, out_ref, w_ref, full_ref, l_ref, crep_ref, z0_ref, z1_ref):
    spread_screens(w4_ref, w_ref)
    fill_columns(m1_ref, full_ref)
    spread = dot3(halves(c_ref[...]), (f_ref[0], f_ref[1]))
    for at in range(4):
        crep_ref[at] = spread[:, 128 * at : 128 * at + 128]

    def clear(step, carry):
        tus = pl.ds(pl.multiple_of(step * 16, 16), 16)
        zero = jnp.zeros((16, 16, 8, 128), F32)
        z0_ref[:, tus] = zero
        z1_ref[:, tus] = zero
        return carry

    lax.fori_loop(0, 16, clear, 0)

    def add(it, carry):
        for k in range(16):
            z_ref = (z0_ref, z1_ref)[k % 2]
            half, row = k // 8, k % 8
            word = idx_ref[it % 32, 0, it // 32 * 16 + k]
            tu, tv = word & 255, word >> 8
            t = (tv >> 2) & 7
            cr = jnp.broadcast_to(crep_ref[2 * half, pl.ds(it * 8 + row, 1), :], (8, 128))
            ci = jnp.broadcast_to(crep_ref[2 * half + 1, pl.ds(it * 8 + row, 1), :], (8, 128))
            wr, wi = w_ref[tv, 0], w_ref[tv, 1]
            z_ref[t, tu] += cr * wr + ci * wi
            z_ref[8 + t, tu] += ci * wr - cr * wi
        return carry

    lax.fori_loop(0, 256, add, 0)

    def stage(step, carry):
        tus = pl.ds(pl.multiple_of(step * 32, 32), 32)
        res = None
        for block in range(8):
            lanes = slice(256 * block, 256 * block + 256)
            parts = [(z0_ref[t, tus] + z1_ref[t, tus]).reshape(256, 128) for t in (2 * block, 2 * block + 1)]
            left = halves(jnp.concatenate(parts, axis=1))
            part = dot3(left, (full_ref[0, :, lanes], full_ref[1, :, lanes]), dot_t)
            res = part if res is None else res + part
        rows = pl.ds(pl.multiple_of(step * 256, 256), 256)
        l_ref[0, rows, :], l_ref[1, rows, :] = res[:, 0:128], res[:, 128:256]
        return carry

    lax.fori_loop(0, 8, stage, 0)

    wide = []
    for at in range(2):
        wide += halves(jnp.concatenate([l_ref[at, pl.ds(b, 256, stride=8), :] for b in range(8)], axis=1))
    cos, sin = (m_ref[0], m_ref[1]), (m_ref[2], m_ref[3])
    twr = jnp.concatenate([tw_ref[0]] * 2, axis=1)
    twi = jnp.concatenate([tw_ref[1]] * 2, axis=1)
    for x in range(4):
        place = placing(x)
        pieces = [dot_t(piece, place).astype(BF16) for piece in wide]
        ur, ui = (pieces[0], pieces[1]), (pieces[2], pieces[3])
        ar = dot3(cos, ur) - dot3(sin, ui)
        ai = dot3(cos, ui) + dot3(sin, ur)
        out_ref[:, x, 0] = (ar * twr + ai * twi).reshape(8, 32, 256)
        out_ref[:, x, 1] = (ai * twr - ar * twi).reshape(8, 32, 256)


def hdot(left, right):
    return jnp.dot(left, right, preferred_element_type=F32, precision=HIGHEST)


def hdot_t(left, right):
    return lax.dot_general(left, right, (((1,), (1,)), ((), ())), preferred_element_type=F32, precision=HIGHEST)


def subgrid_kernel(t_ref, right_ref, left_ref, wa_ref, wb_ref, pa_ref, pb_ref, obs_ref, live_ref, vis_ref, g_ref, out_ref, send1, recv1, sendr, recvr, sendl, recvl):
    slab, z, x, own = greet(True, True)
    tiles = jnp.concatenate([t_ref[pl.ds(k, 32, stride=8), :] for k in range(8)], axis=0)
    both = hdot(tiles, right_ref[...])
    rows = []
    for k in range(8):
        cut = slice(32 * k, 32 * k + 32)
        y, iy = both[cut, 0:128], both[cut, 128:256]
        column = jnp.concatenate([jnp.concatenate([y, iy], axis=1), jnp.concatenate([iy, -y], axis=1)], axis=0)
        s_both = hdot(left_ref[0], column)
        s, i_s = s_both[:, 0:128], s_both[:, 128:256]
        wa, wb = wa_ref[k], wb_ref[k]
        weighted = wa * s + wb * i_s
        found, i_found = [], []
        for half in range(2):
            at = k + 8 * half
            ar, ai = pa_ref[0, at], pa_ref[1, at]
            br, bi = pb_ref[0, at], pb_ref[1, at]
            phase = jnp.concatenate([jnp.concatenate([br, bi], axis=1), jnp.concatenate([-bi, br], axis=1)], axis=0)
            part = hdot(weighted[:, 64 * half : 64 * half + 64], phase)
            pr, pi = part[:, 0:128], part[:, 128:256]
            live = live_ref[pl.ds(at, 1), :]
            rr = (obs_ref[pl.ds(2 * at, 1), :] - jnp.sum(ar * pr - ai * pi, axis=0, keepdims=True)) * live
            ri = (obs_ref[pl.ds(2 * at + 1, 1), :] - jnp.sum(ar * pi + ai * pr, axis=0, keepdims=True)) * live
            vis_ref[pl.ds(2 * at, 1), :] = rr
            vis_ref[pl.ds(2 * at + 1, 1), :] = ri
            sr, si = ar * rr + ai * ri, ar * ri - ai * rr
            sent = jnp.concatenate([jnp.concatenate([sr, si], axis=1), jnp.concatenate([-si, sr], axis=1)], axis=0)
            back = hdot_t(sent, phase)
            found.append(back[0:32])
            i_found.append(back[32:64])
        c, ic = jnp.concatenate(found, axis=1), jnp.concatenate(i_found, axis=1)
        r, ir = wa * c - wb * ic, wa * ic + wb * c
        rows.append(hdot(left_ref[1], jnp.concatenate([r, ir], axis=0)))
    tile = hdot_t(jnp.concatenate(rows, axis=0), right_ref[:, 0:128])
    for k in range(8):
        out_ref[pl.ds(k, 32, stride=8), :] = tile[32 * k : 32 * k + 32]

    def block(d):
        return pl.ds(pl.multiple_of(8 * d, 8), 8)

    def plane_copy(d):
        peer = (own + d) % 32
        return remote(out_ref.at[block(peer)], g_ref.at[z, block(own)], send1.at[d], recv1.at[own], place_of(peer, z))

    def plane_wait(d):
        peer = (own + d) % 32
        remote(out_ref.at[block(peer)], g_ref.at[z, block(peer)], send1.at[d], recv1.at[peer], place_of(peer, z)).wait_recv()

    each(32, lambda d: plane_copy(d).start())
    g_ref[z, block(own), :] = out_ref[block(own), :]
    each(32, plane_wait)

    def right_copy(h, u):
        ref = g_ref.at[(z + 8 - h) % 8, pl.ds(64 * u, 64)]
        return remote(ref, ref, sendr.at[h, u], recvr.at[h, u], (slab, (z + 1) % 8, x))

    def left_copy(h, u):
        ref = g_ref.at[(z + h) % 8, pl.ds(64 * u, 64)]
        return remote(ref, ref, sendl.at[h, u], recvl.at[h, u], (slab, (z + 7) % 8, x))

    def right_wait(h, u):
        ref = g_ref.at[(z + 7 - h) % 8, pl.ds(64 * u, 64)]
        remote(ref, ref, sendr.at[h, u], recvr.at[h, u], (slab, (z + 1) % 8, x)).wait_recv()

    def left_wait(h, u):
        ref = g_ref.at[(z + 1 + h) % 8, pl.ds(64 * u, 64)]
        remote(ref, ref, sendl.at[h, u], recvl.at[h, u], (slab, (z + 7) % 8, x)).wait_recv()

    for h in range(4):
        for u in range(4):
            if h:
                right_wait(h - 1, u)
            right_copy(h, u).start()
            if h < 3:
                if h:
                    left_wait(h - 1, u)
                left_copy(h, u).start()
    for u in range(4):
        left_wait(2, u)
        right_wait(3, u)
    each(32, lambda d: plane_copy(d).wait_send())
    for u in range(4):
        for h in range(4):
            right_copy(h, u).wait_send()
            if h < 3:
                left_copy(h, u).wait_send()


def subgrid_tables():
    index = np.arange(SUB)
    cos, sin = unit(index[:, None] * (index[None, :] - SUB // 2), SUB)
    one = np.block([[cos, sin], [-sin, cos]])
    turned = np.block([[-sin, cos], [-cos, -sin]])
    zero = np.zeros_like(one)
    right = np.concatenate([np.block([[one, zero], [zero, one]]), np.block([[turned, zero], [zero, turned]])], axis=1)
    left = np.stack([np.concatenate([cos.T, sin.T], axis=1), np.concatenate([cos, -sin], axis=1)])
    return right.astype(np.float32), (left / (SUB * SUB)).astype(np.float32)


def phases(coords):
    offsets = (jnp.arange(SUB, dtype=jnp.int32) - SUB // 2).astype(F32)
    along = (-2.0 * math.pi / SUB) * coords[:, None, :] * offsets[None, :, None]
    return jnp.stack([jnp.cos(along), jnp.sin(along)])


def in_vmem(count):
    return [pl.BlockSpec(memory_space=pltpu.VMEM)] * count


def call(kernel, out, specs, scratch=(), collective_id=None, out_specs=None):
    return pl.pallas_call(
        kernel,
        out_shape=out,
        in_specs=specs,
        out_specs=out_specs or jax.tree.map(lambda _: pl.BlockSpec(memory_space=pltpu.VMEM), out),
        scratch_shapes=list(scratch),
        compiler_params=pltpu.CompilerParams(
            vmem_limit_bytes=VMEM_LIMIT, collective_id=collective_id, has_side_effects=collective_id is not None
        ),
    )


def f32(*shape):
    return jax.ShapeDtypeStruct(shape, F32)


SMEM = pl.BlockSpec(memory_space=pltpu.SMEM)


def per_device(model_image, vis_coords, vis_observed, tile_slot, tile_group, w_plane, vis_count):
    slab, z, x = (lax.axis_index(a) for a in SLAB_BL)
    word = tile_slot + 256 * (32 * slab + tile_group[:, 0])
    lane = jnp.arange(128, dtype=jnp.int32)
    word_row = jnp.where(lane // 16 == z, jnp.tile(word, 8), 0).reshape(1, 128)
    own = slab * 4 + x
    angle = (2.0 * math.pi / N) * (own * jnp.arange(256, dtype=jnp.int32)).astype(F32)
    tw = jnp.broadcast_to(jnp.stack([jnp.cos(angle), -jnp.sin(angle)])[:, :, None], (2, 256, 128))
    j = jnp.arange(128, dtype=jnp.int32)
    shift = (2.0 * math.pi / 8.0) * (j * z % 8).astype(F32)
    phz = jnp.stack([jnp.cos(shift), -jnp.sin(shift)]) / N
    half, part, jj = j // 64, j // 32 % 2, j % 32
    n = jnp.arange(512, dtype=jnp.int32)
    n_half, n_part, n_jj = n // 256, n // 128 % 2, n % 32
    same = (half[:, None] == n_half[None, :]) & (jj[:, None] == n_jj[None, :])
    pick = jnp.where(part[:, None] == n_part[None, :], phz[0][:, None], jnp.where(part[:, None] == 0, -phz[1][:, None], phz[1][:, None]))
    spread = jnp.where(same, pick, 0.0)
    spread = jnp.stack(halves(spread))
    pa, pb = phases(vis_coords[:, 0, :]), phases(vis_coords[:, 1, :])
    mm = (jnp.arange(SUB, dtype=jnp.int32) - SUB // 2).astype(F32)
    radius = (mm[:, None] ** 2 + mm[None, :] ** 2) / (SUB // 2) ** 2
    turned = -W_STEP * w_plane.astype(F32)[:, None, None] * radius[None]
    lanes = lambda value: jnp.concatenate([value[:8], value[:8], value[8:], value[8:]], axis=2)
    wa, wb = lanes(jnp.cos(turned)), lanes(jnp.sin(turned))
    live = (jnp.arange(128, dtype=jnp.int32)[None, :] < vis_count[:, None]).astype(F32)
    rows, columns, screens = row_tables(), column_tables(), screen_tables()
    right, left = subgrid_tables()

    a, words = call(
        forward_kernel,
        (f32(32, 2, 32, 256), jax.ShapeDtypeStruct((32, 1, 128), jnp.int32)),
        [ANY] + in_vmem(1),
        [
            pltpu.VMEM((8, 2, 4, 32, 256), F32),
            pltpu.VMEM((32, 2, 32, 256), F32),
            pltpu.VMEM((8, 1, 128), jnp.int32),
            pltpu.VMEM((1, 128), jnp.int32),
            DMA,
            DMA((4, 8)),
            DMA((4, 8)),
            DMA((4, 32)),
            DMA((4, 32)),
            DMA((8,)),
            DMA((8,)),
            DMA((32,)),
            DMA((32,)),
        ],
        collective_id=0,
    )(model_image.reshape(2, 4, 8, 32, 256), word_row)
    a = a.reshape(8, 4, 2, 32, 256)
    partial = call(
        gather_kernel,
        f32(2048, 128),
        [SMEM] + in_vmem(6),
        [
            pltpu.VMEM((256, 2, 8, 128), F32),
            pltpu.VMEM((2, 256, 2048), BF16),
            pltpu.VMEM((2, 2048, 128), F32),
            pltpu.VMEM((2, 2048, 128), F32),
            pltpu.VMEM((16, 256, 8, 128), F32),
        ],
    )(words, a, tw, rows, columns, screens, phz)
    summed = lax.psum_scatter(partial.reshape(8, 256, 128), "bl_0", scatter_dimension=0, tiled=True)
    tiles = lax.all_to_all(summed.reshape(32, 8, 128), PLANE, split_axis=0, concat_axis=0, tiled=True)
    vis, every = call(
        subgrid_kernel,
        (f32(32, 128), f32(8, 256, 128)),
        in_vmem(9),
        [pltpu.VMEM((256, 128), F32), DMA((32,)), DMA((32,)), DMA((4, 4)), DMA((4, 4)), DMA((3, 4)), DMA((3, 4))],
        collective_id=1,
    )(
        tiles.reshape(256, 128), right, left, wa, wb, pa, pb, vis_observed.reshape(32, 128), live
    )
    every = every.reshape(2048, 128)
    spots = call(
        scatter_kernel,
        f32(8, 4, 2, 32, 256),
        [SMEM] + in_vmem(6),
        [
            pltpu.VMEM((256, 2, 8, 128), F32),
            pltpu.VMEM((2, 256, 2048), BF16),
            pltpu.VMEM((2, 2048, 128), F32),
            pltpu.VMEM((4, 2048, 128), F32),
            pltpu.VMEM((16, 256, 8, 128), F32),
            pltpu.VMEM((16, 256, 8, 128), F32),
        ],
    )(words, every, tw, rows, columns, screens, spread)
    image = call(
        backward_kernel,
        f32(2, 4, 8, 32, 256),
        [ANY],
        [
            pltpu.VMEM((32, 2, 32, 256), F32),
            pltpu.VMEM((8, 2, 4, 32, 256), F32),
            DMA,
            DMA((4,)),
            DMA((4, 32)),
            DMA((4, 32)),
            DMA((4, 8)),
            DMA((4, 8)),
        ],
        collective_id=2,
        out_specs=ANY,
    )(spots.reshape(32, 2, 32, 256)).reshape(2, 1024, 256)
    return image, vis.reshape(16, 2, 128)


def solution(mesh):
    torus = Mesh(mesh.devices.reshape(mesh.shape["slab"], 8, 4), SLAB_BL)
    in_specs = (
        P(None, "slab", BL),
        P(SLAB_BL, None, None),
        P(SLAB_BL, None, None),
        P(SLAB_BL),
        P(SLAB_BL, None),
        P(SLAB_BL),
        P(SLAB_BL),
    )
    out_specs = (P(None, "slab", BL), P(SLAB_BL, None, None))
    return jax.shard_map(per_device, mesh=torus, in_specs=in_specs, out_specs=out_specs, check_vma=False)
```

```python
import functools
import math

import jax
import jax.numpy as jnp
import numpy as np
from jax import lax
from jax.experimental import pallas as pl
from jax.experimental.pallas import tpu as pltpu
from jax.sharding import Mesh
from jax.sharding import PartitionSpec as P

N = 8192
SUB = 32
BL = ("bl_0", "bl_1")
SLAB_BL = ("slab", "bl_0", "bl_1")
PLANE = ("slab", "bl_1")
W_STEP = 0.1
F32 = jnp.float32
BF16 = jnp.bfloat16
HIGHEST = lax.Precision.HIGHEST
MESH = pl.DeviceIdType.MESH
ANY = pl.BlockSpec(memory_space=pl.ANY)
DMA = pltpu.SemaphoreType.DMA
VMEM_LIMIT = 62 * 1024 * 1024


def unit(numerator, modulus):
    angle = 2.0 * np.pi * (numerator % modulus) / modulus
    return np.cos(angle), np.sin(angle)


def halves(value):
    high = value.astype(BF16)
    return high, (value - high.astype(F32)).astype(BF16)


def np_halves(value):
    value = np.asarray(value, np.float32)
    high = value.astype(BF16)
    return np.stack([high, (value - high.astype(np.float32)).astype(BF16)])


def row_tables():
    index = np.arange(256)
    cos, sin = unit(np.outer(index, index), 256)
    return np.concatenate([np_halves(cos), np_halves(sin)])


def column_tables():
    a = np.arange(128)[:, None]
    v = np.arange(1024)[None, :]
    cos, sin = unit(a * v, 1024)
    return np.concatenate([np_halves(cos), np_halves(sin)])


def screen_tables():
    b = np.arange(8)[:, None]
    v = np.arange(N)[None, :]
    cos, sin = unit(b * v, N)
    both = np.stack([cos, -sin]).reshape(2, 8, 64, 128)
    return both.transpose(2, 0, 1, 3).astype(np.float32)


def dot(left, right):
    return jnp.dot(left, right, preferred_element_type=F32)


def dot_t(left, right):
    return lax.dot_general(left, right, (((1,), (1,)), ((), ())), preferred_element_type=F32)


def dot3(left, right, product=dot):
    return product(left[0], right[0]) + (product(left[0], right[1]) + product(left[1], right[0]))


def dft4(values, sign):
    (ar, ai), (br, bi), (cr, ci), (dr, di) = values
    pr, pi, mr, mi = ar + cr, ai + ci, ar - cr, ai - ci
    qr, qi, nr, ni = br + dr, bi + di, br - dr, bi - di
    return [
        (pr + qr, pi + qi),
        (mr - sign * ni, mi + sign * nr),
        (pr - qr, pi - qi),
        (mr + sign * ni, mi - sign * nr),
    ]


def turn(value, numerator, modulus, sign):
    cos, sin = math.cos(2 * math.pi * numerator / modulus), sign * math.sin(2 * math.pi * numerator / modulus)
    if numerator % modulus == 0:
        return value
    re, im = value
    return (re * cos - im * sin, re * sin + im * cos)


def dft8(values, sign):
    even, odd = dft4(values[0::2], sign), dft4(values[1::2], sign)
    out = [None] * 8
    for k in range(4):
        tr, ti = turn(odd[k], k, 8, sign)
        out[k] = (even[k][0] + tr, even[k][1] + ti)
        out[k + 4] = (even[k][0] - tr, even[k][1] - ti)
    return out


def butterfly(v_ref, w_ref, c):
    def tile(step, carry):
        rows = pl.ds(pl.multiple_of(32 // CHUNKS * c + step // 2 * 8, 8), 8)
        lanes = pl.ds(pl.multiple_of(step % 2 * 128, 128), 128)
        mid = []
        for b in range(4):
            column = dft8([(v_ref[s, 0, b, rows, lanes], v_ref[s, 1, b, rows, lanes]) for s in range(8)], -1.0)
            mid.append([turn(column[i0], i0 * b, 32, -1.0) for i0 in range(8)])
        for i0 in range(8):
            done = dft4([mid[b][i0] for b in range(4)], -1.0)
            for i1 in range(4):
                w_ref[i0 + 8 * i1, 0, rows, lanes] = done[i1][0]
                w_ref[i0 + 8 * i1, 1, rows, lanes] = done[i1][1]
        return carry

    lax.fori_loop(0, 8 // CHUNKS, tile, 0)


def unbutterfly(w_ref, v_ref, c):
    def tile(step, carry):
        rows = pl.ds(pl.multiple_of(32 // CHUNKS * c + step // 2 * 8, 8), 8)
        lanes = pl.ds(pl.multiple_of(step % 2 * 128, 128), 128)
        mid = []
        for i0 in range(8):
            column = dft4([(w_ref[i0 + 8 * i1, 0, rows, lanes], w_ref[i0 + 8 * i1, 1, rows, lanes]) for i1 in range(4)], 1.0)
            mid.append([turn(column[b], i0 * b, 32, 1.0) for b in range(4)])
        for b in range(4):
            done = dft8([mid[i0][b] for i0 in range(8)], 1.0)
            for s in range(8):
                v_ref[s, 0, b, rows, lanes] = done[s][0]
                v_ref[s, 1, b, rows, lanes] = done[s][1]
        return carry

    lax.fori_loop(0, 8 // CHUNKS, tile, 0)


def remote(src, dst, send, recv, device):
    return pltpu.make_async_remote_copy(
        src_ref=src, dst_ref=dst, send_sem=send, recv_sem=recv, device_id=device, device_id_type=MESH
    )


def each(count, body):
    def step(at, carry):
        body(at)
        return carry

    lax.fori_loop(1, count, step, 0)


def place_of(peer, z):
    return (peer // 4, z, peer % 4)


def greet(plane, along_z):
    slab, z, x = (lax.axis_index(a) for a in SLAB_BL)
    own = slab * 4 + x
    barrier = pltpu.get_barrier_semaphore()
    if plane:
        each(32, lambda d: pl.semaphore_signal(barrier, inc=1, device_id=place_of((own + d) % 32, z), device_id_type=MESH))
    if along_z:
        each(8, lambda d: pl.semaphore_signal(barrier, inc=1, device_id=(slab, (z + d) % 8, x), device_id_type=MESH))
    pl.semaphore_wait(barrier, 31 * plane + 7 * along_z)
    return slab, z, x, own


CHUNKS = 2
STEP8 = 3
STEP32 = 13


def chunk(c):
    return pl.ds(32 // CHUNKS * c, 32 // CHUNKS)


def forward_kernel(image_ref, word_ref, a_ref, idx_ref, v_ref, w_ref, zrow_ref, row_ref, local, send1, recv1, send2, recv2, sendz, recvz, sendi, recvi):
    slab, z, x, own = greet(True, True)

    def word_copy(d):
        peer = (z + d) % 8
        return remote(word_ref, zrow_ref.at[z], sendz.at[d], recvz.at[z], (slab, peer, x))

    def slab_copy(c, d):
        peer = (slab + STEP8 * d) % 8
        return remote(image_ref.at[:, :, peer, chunk(c)], v_ref.at[slab, :, :, chunk(c)], send1.at[c, d], recv1.at[c, slab], (peer, z, x))

    def slab_wait(c, d):
        peer = (slab + STEP8 * d) % 8
        remote(image_ref.at[:, :, peer, chunk(c)], v_ref.at[peer, :, :, chunk(c)], send1.at[c, d], recv1.at[c, peer], (peer, z, x)).wait_recv()

    def plane_copy(c, d):
        peer = (own + STEP32 * d) % 32
        return remote(w_ref.at[peer, :, chunk(c)], a_ref.at[own, :, chunk(c)], send2.at[c, d], recv2.at[c, own], place_of(peer, z))

    def plane_wait(c, d):
        peer = (own + STEP32 * d) % 32
        remote(w_ref.at[peer, :, chunk(c)], a_ref.at[peer, :, chunk(c)], send2.at[c, d], recv2.at[c, peer], place_of(peer, z)).wait_recv()

    def row_copy(d):
        return remote(row_ref, idx_ref.at[own], sendi.at[d], recvi.at[own], place_of((own + d) % 32, z))

    each(8, lambda d: word_copy(d).start())
    mine = pltpu.make_async_copy(image_ref.at[:, :, slab], v_ref.at[slab], local)
    mine.start()
    for c in range(CHUNKS):
        each(8, lambda d: slab_copy(c, d).start())

    def word_wait(d):
        peer = (z + d) % 8
        remote(word_ref, zrow_ref.at[peer], sendz.at[d], recvz.at[peer], (slab, peer, x)).wait_recv()

    each(8, word_wait)
    zrow_ref[z] = word_ref[...]
    row = zrow_ref[0]
    for at in range(1, 8):
        row = row + zrow_ref[at]
    row_ref[...] = row
    idx_ref[own] = row
    mine.wait()
    for c in range(CHUNKS):
        each(8, lambda d: slab_wait(c, d))
        if c == 0:
            each(32, lambda d: row_copy(d).start())
        butterfly(v_ref, w_ref, c)
        each(32, lambda d: plane_copy(c, d).start())
        a_ref[own, :, chunk(c)] = w_ref[own, :, chunk(c)]

    def row_wait(d):
        peer = (own + STEP32 * d) % 32
        remote(row_ref, idx_ref.at[peer], sendi.at[d], recvi.at[peer], place_of(peer, z)).wait_recv()

    each(32, row_wait)
    for c in range(CHUNKS):
        each(32, lambda d: plane_wait(c, d))
    each(8, lambda d: word_copy(d).wait_send())
    each(32, lambda d: row_copy(d).wait_send())
    for c in range(CHUNKS):
        each(8, lambda d: slab_copy(c, d).wait_send())
        each(32, lambda d: plane_copy(c, d).wait_send())


def backward_kernel(spot_ref, out_ref, w_ref, v_ref, local, keep, send1, recv1, send2, recv2):
    slab, z, x, own = greet(True, False)

    def plane_copy(c, d):
        peer = (own + STEP32 * d) % 32
        return remote(spot_ref.at[peer, :, chunk(c)], w_ref.at[own, :, chunk(c)], send1.at[c, d], recv1.at[c, own], place_of(peer, z))

    def plane_wait(c, d):
        peer = (own + STEP32 * d) % 32
        remote(spot_ref.at[peer, :, chunk(c)], w_ref.at[peer, :, chunk(c)], send1.at[c, d], recv1.at[c, peer], place_of(peer, z)).wait_recv()

    def slab_copy(c, d):
        peer = (slab + STEP8 * d) % 8
        return remote(v_ref.at[peer, :, :, chunk(c)], out_ref.at[:, :, slab, chunk(c)], send2.at[c, d], recv2.at[c, slab], (peer, z, x))

    def slab_wait(c, d):
        peer = (slab + STEP8 * d) % 8
        remote(v_ref.at[peer, :, :, chunk(c)], out_ref.at[:, :, peer, chunk(c)], send2.at[c, d], recv2.at[c, peer], (peer, z, x)).wait_recv()

    mine = pltpu.make_async_copy(spot_ref.at[own], w_ref.at[own], local)
    mine.start()
    for c in range(CHUNKS):
        each(32, lambda d: plane_copy(c, d).start())
    mine.wait()
    kept = []
    for c in range(CHUNKS):
        each(32, lambda d: plane_wait(c, d))
        unbutterfly(w_ref, v_ref, c)
        each(8, lambda d: slab_copy(c, d).start())
        copy = pltpu.make_async_copy(v_ref.at[slab, :, :, chunk(c)], out_ref.at[:, :, slab, chunk(c)], keep.at[c])
        copy.start()
        kept.append(copy)
    for c in range(CHUNKS):
        each(8, lambda d: slab_wait(c, d))
        kept[c].wait()
    for c in range(CHUNKS):
        each(32, lambda d: plane_copy(c, d).wait_send())
        each(8, lambda d: slab_copy(c, d).wait_send())


def placing(x):
    c0 = lax.broadcasted_iota(jnp.int32, (256, 1024), 0)
    n = lax.broadcasted_iota(jnp.int32, (256, 1024), 1)
    hit = (c0 == 8 * (n & 31) + (n >> 7)) & (((n >> 5) & 3) == x)
    return jnp.where(hit, 1.0, 0.0).astype(BF16)


def spread_screens(w4_ref, w_ref):
    group = lax.broadcasted_iota(jnp.int32, (8, 128), 1) >> 5

    def expand(q, carry):
        for m in range(4):
            mask = group == m
            w_ref[4 * q + m, 0] = jnp.where(mask, w4_ref[q, 0], 0.0)
            w_ref[4 * q + m, 1] = jnp.where(mask, w4_ref[q, 1], 0.0)
        return carry

    lax.fori_loop(0, 64, expand, 0)


def fill_columns(m1_ref, full_ref):
    for h in range(2):
        cos, sin = m1_ref[h], m1_ref[2 + h]
        full_ref[h, 0:128, 0:1024] = cos
        full_ref[h, 0:128, 1024:2048] = -sin
        full_ref[h, 128:256, 0:1024] = sin
        full_ref[h, 128:256, 1024:2048] = cos


def row_sums(values):
    at = lax.broadcasted_iota(jnp.int32, (8, 128), 0)
    quads = []
    for r in range(4):
        first, second = values[r], values[r + 4]
        quads.append(jnp.where(at < 4, first, second) + pltpu.roll(jnp.where(at < 4, second, first), 4, 0))
    pairs = []
    for r in range(2):
        first, second = quads[r] + pltpu.roll(quads[r], 6, 0), quads[r + 2] + pltpu.roll(quads[r + 2], 2, 0)
        pairs.append(jnp.where(at & 2 == 0, first, second))
    first, second = pairs[0] + pltpu.roll(pairs[0], 7, 0), pairs[1] + pltpu.roll(pairs[1], 1, 0)
    return jnp.where(at & 1 == 0, first, second)


def gather_kernel(
    idx_ref, a_ref, tw_ref, m_ref, m1_ref, w4_ref, f_ref, out_ref,
    w_ref, full_ref, high_ref, low_ref, z_ref, s_ref, part_ref, got_ref, sum_ref, sendz, recvz, sendp, recvp,
):
    slab, z, x, own = greet(True, True)
    spread_screens(w4_ref, w_ref)
    fill_columns(m1_ref, full_ref)
    cos, sin = (m_ref[0], m_ref[1]), (m_ref[2], m_ref[3])
    twr = jnp.concatenate([tw_ref[0]] * 2, axis=1)
    twi = jnp.concatenate([tw_ref[1]] * 2, axis=1)
    total = [None] * 4
    for xx in range(4):
        ar = a_ref[:, xx, 0].reshape(256, 256)
        ai = a_ref[:, xx, 1].reshape(256, 256)
        br, bi = halves(ar * twr - ai * twi), halves(ar * twi + ai * twr)
        ur = dot3(cos, br) + dot3(sin, bi)
        ui = dot3(cos, bi) - dot3(sin, br)
        place = placing(xx)
        for at, piece in enumerate(halves(ur) + halves(ui)):
            part = dot(piece, place)
            total[at] = part if total[at] is None else total[at] + part
    for b in range(8):
        cut = slice(128 * b, 128 * b + 128)
        rows = pl.ds(b, 256, stride=8)
        for part in range(2):
            high_ref[part, rows, :] = total[2 * part][:, cut]
            low_ref[part, rows, :] = total[2 * part + 1][:, cut]

    def stage(step, carry):
        block, part = step // 4, step % 4
        rows = pl.ds(pl.multiple_of(part * 512, 512), 512)
        lanes = pl.ds(pl.multiple_of(block * 256, 256), 256)
        left = tuple(jnp.concatenate([ref[0, rows, :], ref[1, rows, :]], axis=1).astype(BF16) for ref in (high_ref, low_ref))
        right = (full_ref[0, :, lanes], full_ref[1, :, lanes])
        res = dot3(left, right)
        z_ref[block // 4, pl.ds(pl.multiple_of(block % 4 * 512 + part * 64, 64), 64)] = res[:, 0:128].reshape(64, 8, 128)
        z_ref[block // 4, pl.ds(pl.multiple_of(block % 4 * 512 + 256 + part * 64, 64), 64)] = res[:, 128:256].reshape(64, 8, 128)
        return carry

    lax.fori_loop(0, 32, stage, 0)

    def collect(zc):
        def some(step, carry):
            for d in (2 * step, 2 * step + 1):
                for half in range(2):
                    res, ims = [], []
                    for k in range(8):
                        word = idx_ref[d, 0, zc * 16 + half * 8 + k]
                        spot, tv = word & 2047, word >> 11
                        zr, zi = z_ref[0, spot], z_ref[1, spot]
                        wr, wi = w_ref[tv, 0], w_ref[tv, 1]
                        res.append(zr * wr - zi * wi)
                        ims.append(zr * wi + zi * wr)
                    rows = pl.ds(pl.multiple_of(d * 8, 8), 8)
                    s_ref[2 * half, rows, :] = row_sums(res)
                    s_ref[2 * half + 1, rows, :] = row_sums(ims)
            return carry

        lax.fori_loop(0, 16, some, 0)
        sums = jnp.concatenate([s_ref[at] for at in range(4)], axis=1)
        part_ref[zc] = dot3(halves(sums), (f_ref[0], f_ref[1]), dot_t)

    def z_copy(d):
        peer = (z + d) % 8
        return remote(part_ref.at[peer], got_ref.at[z], sendz.at[d], recvz.at[z], (slab, peer, x))

    def z_wait(d):
        peer = (z + d) % 8
        remote(part_ref.at[peer], got_ref.at[peer], sendz.at[d], recvz.at[peer], (slab, peer, x)).wait_recv()

    def outward(step, carry):
        d = 4 + (1 - 2 * (step % 2)) * ((step + 1) // 2)
        d = 8 - d
        collect((z + d) % 8)
        z_copy(d).start()
        return carry

    lax.fori_loop(0, 7, outward, 0)
    collect(z)
    each(8, z_wait)
    total = part_ref[z]
    for d in range(1, 8):
        total = total + got_ref[(z + d) % 8]
    sum_ref[...] = total

    def block(d):
        return pl.ds(pl.multiple_of(8 * d, 8), 8)

    def plane_copy(d):
        peer = (own + STEP32 * d) % 32
        return remote(sum_ref.at[block(peer)], out_ref.at[block(own)], sendp.at[d], recvp.at[own], place_of(peer, z))

    def plane_wait(d):
        peer = (own + STEP32 * d) % 32
        remote(sum_ref.at[block(peer)], out_ref.at[block(peer)], sendp.at[d], recvp.at[peer], place_of(peer, z)).wait_recv()

    each(32, lambda d: plane_copy(d).start())
    out_ref[block(own), :] = sum_ref[block(own), :]
    each(32, plane_wait)
    each(8, lambda d: z_copy(d).wait_send())
    each(32, lambda d: plane_copy(d).wait_send())


def scatter_kernel(idx_ref, c_ref, tw_ref, m_ref, m1_ref, w4_ref, f_ref, out_ref, w_ref, full_ref, l_ref, crep_ref, z0_ref, z1_ref):
    spread_screens(w4_ref, w_ref)
    fill_columns(m1_ref, full_ref)
    spread = dot3(halves(c_ref[...]), (f_ref[0], f_ref[1]))
    for at in range(4):
        crep_ref[at] = spread[:, 128 * at : 128 * at + 128]

    def clear(step, carry):
        spots = pl.ds(pl.multiple_of(step * 128, 128), 128)
        zero = jnp.zeros((2, 128, 8, 128), F32)
        z0_ref[:, spots] = zero
        z1_ref[:, spots] = zero
        return carry

    lax.fori_loop(0, 16, clear, 0)

    def add(it, carry):
        for k in range(16):
            z_ref = (z0_ref, z1_ref)[k % 2]
            half, row = k // 8, k % 8
            word = idx_ref[it % 32, 0, it // 32 * 16 + k]
            spot, tv = word & 2047, word >> 11
            cr = jnp.broadcast_to(crep_ref[2 * half, pl.ds(it * 8 + row, 1), :], (8, 128))
            ci = jnp.broadcast_to(crep_ref[2 * half + 1, pl.ds(it * 8 + row, 1), :], (8, 128))
            wr, wi = w_ref[tv, 0], w_ref[tv, 1]
            z_ref[0, spot] += cr * wr + ci * wi
            z_ref[1, spot] += ci * wr - cr * wi
        return carry

    lax.fori_loop(0, 256, add, 0)

    def stage(step, carry):
        res = None
        for block in range(8):
            lanes = slice(256 * block, 256 * block + 256)
            spots = [pl.ds(pl.multiple_of(t % 8 * 256 + step * 32, 32), 32) for t in (2 * block, 2 * block + 1)]
            parts = [(z0_ref[block // 4, at] + z1_ref[block // 4, at]).reshape(256, 128) for at in spots]
            left = halves(jnp.concatenate(parts, axis=1))
            part = dot3(left, (full_ref[0, :, lanes], full_ref[1, :, lanes]), dot_t)
            res = part if res is None else res + part
        rows = pl.ds(pl.multiple_of(step * 256, 256), 256)
        l_ref[0, rows, :], l_ref[1, rows, :] = res[:, 0:128], res[:, 128:256]
        return carry

    lax.fori_loop(0, 8, stage, 0)

    wide = []
    for at in range(2):
        wide += halves(jnp.concatenate([l_ref[at, pl.ds(b, 256, stride=8), :] for b in range(8)], axis=1))
    cos, sin = (m_ref[0], m_ref[1]), (m_ref[2], m_ref[3])
    twr = jnp.concatenate([tw_ref[0]] * 2, axis=1)
    twi = jnp.concatenate([tw_ref[1]] * 2, axis=1)
    for x in range(4):
        place = placing(x)
        pieces = [dot_t(piece, place).astype(BF16) for piece in wide]
        ur, ui = (pieces[0], pieces[1]), (pieces[2], pieces[3])
        ar = dot3(cos, ur) - dot3(sin, ui)
        ai = dot3(cos, ui) + dot3(sin, ur)
        out_ref[:, x, 0] = (ar * twr + ai * twi).reshape(8, 32, 256)
        out_ref[:, x, 1] = (ai * twr - ar * twi).reshape(8, 32, 256)


def hdot(left, right):
    return jnp.dot(left, right, preferred_element_type=F32, precision=HIGHEST)


def hdot_t(left, right):
    return lax.dot_general(left, right, (((1,), (1,)), ((), ())), preferred_element_type=F32, precision=HIGHEST)


def subgrid_kernel(t_ref, right_ref, left_ref, wa_ref, wb_ref, pa_ref, pb_ref, obs_ref, live_ref, vis_ref, g_ref, out_ref, send1, recv1, sendr, recvr, sendl, recvl):
    slab, z, x, own = greet(True, True)
    tiles = jnp.concatenate([t_ref[pl.ds(k, 32, stride=8), :] for k in range(8)], axis=0)
    both = hdot(tiles, right_ref[...])
    rows = []
    for k in range(8):
        cut = slice(32 * k, 32 * k + 32)
        y, iy = both[cut, 0:128], both[cut, 128:256]
        column = jnp.concatenate([jnp.concatenate([y, iy], axis=1), jnp.concatenate([iy, -y], axis=1)], axis=0)
        s_both = hdot(left_ref[0], column)
        s, i_s = s_both[:, 0:128], s_both[:, 128:256]
        wa, wb = wa_ref[k], wb_ref[k]
        weighted = wa * s + wb * i_s
        found, i_found = [], []
        for half in range(2):
            at = k + 8 * half
            ar, ai = pa_ref[0, at], pa_ref[1, at]
            br, bi = pb_ref[0, at], pb_ref[1, at]
            phase = jnp.concatenate([jnp.concatenate([br, bi], axis=1), jnp.concatenate([-bi, br], axis=1)], axis=0)
            part = hdot(weighted[:, 64 * half : 64 * half + 64], phase)
            pr, pi = part[:, 0:128], part[:, 128:256]
            live = live_ref[pl.ds(at, 1), :]
            rr = (obs_ref[pl.ds(2 * at, 1), :] - jnp.sum(ar * pr - ai * pi, axis=0, keepdims=True)) * live
            ri = (obs_ref[pl.ds(2 * at + 1, 1), :] - jnp.sum(ar * pi + ai * pr, axis=0, keepdims=True)) * live
            vis_ref[pl.ds(2 * at, 1), :] = rr
            vis_ref[pl.ds(2 * at + 1, 1), :] = ri
            sr, si = ar * rr + ai * ri, ar * ri - ai * rr
            sent = jnp.concatenate([jnp.concatenate([sr, si], axis=1), jnp.concatenate([-si, sr], axis=1)], axis=0)
            back = hdot_t(sent, phase)
            found.append(back[0:32])
            i_found.append(back[32:64])
        c, ic = jnp.concatenate(found, axis=1), jnp.concatenate(i_found, axis=1)
        r, ir = wa * c - wb * ic, wa * ic + wb * c
        rows.append(hdot(left_ref[1], jnp.concatenate([r, ir], axis=0)))
    tile = hdot_t(jnp.concatenate(rows, axis=0), right_ref[:, 0:128])
    for k in range(8):
        out_ref[pl.ds(k, 32, stride=8), :] = tile[32 * k : 32 * k + 32]

    def block(d):
        return pl.ds(pl.multiple_of(8 * d, 8), 8)

    def plane_copy(d):
        peer = (own + STEP32 * d) % 32
        return remote(out_ref.at[block(peer)], g_ref.at[z, block(own)], send1.at[d], recv1.at[own], place_of(peer, z))

    def plane_wait(d):
        peer = (own + STEP32 * d) % 32
        remote(out_ref.at[block(peer)], g_ref.at[z, block(peer)], send1.at[d], recv1.at[peer], place_of(peer, z)).wait_recv()

    each(32, lambda d: plane_copy(d).start())
    g_ref[z, block(own), :] = out_ref[block(own), :]
    each(32, plane_wait)

    def right_copy(h, u):
        ref = g_ref.at[(z + 8 - h) % 8, pl.ds(64 * u, 64)]
        return remote(ref, ref, sendr.at[h, u], recvr.at[h, u], (slab, (z + 1) % 8, x))

    def left_copy(h, u):
        ref = g_ref.at[(z + h) % 8, pl.ds(64 * u, 64)]
        return remote(ref, ref, sendl.at[h, u], recvl.at[h, u], (slab, (z + 7) % 8, x))

    def right_wait(h, u):
        ref = g_ref.at[(z + 7 - h) % 8, pl.ds(64 * u, 64)]
        remote(ref, ref, sendr.at[h, u], recvr.at[h, u], (slab, (z + 1) % 8, x)).wait_recv()

    def left_wait(h, u):
        ref = g_ref.at[(z + 1 + h) % 8, pl.ds(64 * u, 64)]
        remote(ref, ref, sendl.at[h, u], recvl.at[h, u], (slab, (z + 7) % 8, x)).wait_recv()

    for h in range(4):
        for u in range(4):
            if h:
                right_wait(h - 1, u)
            right_copy(h, u).start()
            if h < 3:
                if h:
                    left_wait(h - 1, u)
                left_copy(h, u).start()
    for u in range(4):
        left_wait(2, u)
        right_wait(3, u)
    each(32, lambda d: plane_copy(d).wait_send())
    for u in range(4):
        for h in range(4):
            right_copy(h, u).wait_send()
            if h < 3:
                left_copy(h, u).wait_send()


def subgrid_tables():
    index = np.arange(SUB)
    cos, sin = unit(index[:, None] * (index[None, :] - SUB // 2), SUB)
    one = np.block([[cos, sin], [-sin, cos]])
    turned = np.block([[-sin, cos], [-cos, -sin]])
    zero = np.zeros_like(one)
    right = np.concatenate([np.block([[one, zero], [zero, one]]), np.block([[turned, zero], [zero, turned]])], axis=1)
    left = np.stack([np.concatenate([cos.T, sin.T], axis=1), np.concatenate([cos, -sin], axis=1)])
    return right.astype(np.float32), (left / (SUB * SUB)).astype(np.float32)


def phases(coords):
    offsets = (jnp.arange(SUB, dtype=jnp.int32) - SUB // 2).astype(F32)
    along = (-2.0 * math.pi / SUB) * coords[:, None, :] * offsets[None, :, None]
    return jnp.stack([jnp.cos(along), jnp.sin(along)])


def in_vmem(count):
    return [pl.BlockSpec(memory_space=pltpu.VMEM)] * count


def call(kernel, out, specs, scratch=(), collective_id=None, out_specs=None):
    return pl.pallas_call(
        kernel,
        out_shape=out,
        in_specs=specs,
        out_specs=out_specs or jax.tree.map(lambda _: pl.BlockSpec(memory_space=pltpu.VMEM), out),
        scratch_shapes=list(scratch),
        compiler_params=pltpu.CompilerParams(
            vmem_limit_bytes=VMEM_LIMIT, collective_id=collective_id, has_side_effects=collective_id is not None
        ),
    )


def f32(*shape):
    return jax.ShapeDtypeStruct(shape, F32)


SMEM = pl.BlockSpec(memory_space=pltpu.SMEM)


def per_device(model_image, vis_coords, vis_observed, tile_slot, tile_group, w_plane, vis_count):
    slab, z, x = (lax.axis_index(a) for a in SLAB_BL)
    tv = 32 * slab + tile_group[:, 0]
    word = tile_slot + 256 * ((tv >> 2) & 7) + 2048 * tv
    lane = jnp.arange(128, dtype=jnp.int32)
    word_row = jnp.where(lane // 16 == z, jnp.tile(word, 8), 0).reshape(1, 128)
    own = slab * 4 + x
    angle = (2.0 * math.pi / N) * (own * jnp.arange(256, dtype=jnp.int32)).astype(F32)
    tw = jnp.broadcast_to(jnp.stack([jnp.cos(angle), -jnp.sin(angle)])[:, :, None], (2, 256, 128))
    j = jnp.arange(128, dtype=jnp.int32)
    shift = (2.0 * math.pi / 8.0) * (j * z % 8).astype(F32)
    phz = jnp.stack([jnp.cos(shift), -jnp.sin(shift)]) / N
    half, part, jj = j // 64, j // 32 % 2, j % 32
    n = jnp.arange(512, dtype=jnp.int32)
    n_half, n_part, n_jj = n // 256, n // 128 % 2, n % 32
    same = (half[:, None] == n_half[None, :]) & (jj[:, None] == n_jj[None, :])
    pick = jnp.where(part[:, None] == n_part[None, :], phz[0][:, None], jnp.where(part[:, None] == 0, -phz[1][:, None], phz[1][:, None]))
    spread = jnp.where(same, pick, 0.0)
    high = lax.reduce_precision(spread, 8, 7)
    spread = jnp.stack([high.astype(BF16), (spread - high).astype(BF16)])
    pa, pb = phases(vis_coords[:, 0, :]), phases(vis_coords[:, 1, :])
    mm = (jnp.arange(SUB, dtype=jnp.int32) - SUB // 2).astype(F32)
    radius = (mm[:, None] ** 2 + mm[None, :] ** 2) / (SUB // 2) ** 2
    turned = -W_STEP * w_plane.astype(F32)[:, None, None] * radius[None]
    lanes = lambda value: jnp.concatenate([value[:8], value[:8], value[8:], value[8:]], axis=2)
    wa, wb = lanes(jnp.cos(turned)), lanes(jnp.sin(turned))
    live = (jnp.arange(128, dtype=jnp.int32)[None, :] < vis_count[:, None]).astype(F32)
    rows, columns, screens = row_tables(), column_tables(), screen_tables()
    right, left = subgrid_tables()

    a, words = call(
        forward_kernel,
        (f32(32, 2, 32, 256), jax.ShapeDtypeStruct((32, 1, 128), jnp.int32)),
        [ANY] + in_vmem(1),
        [
            pltpu.VMEM((8, 2, 4, 32, 256), F32),
            pltpu.VMEM((32, 2, 32, 256), F32),
            pltpu.VMEM((8, 1, 128), jnp.int32),
            pltpu.VMEM((1, 128), jnp.int32),
            DMA,
            DMA((CHUNKS, 8)),
            DMA((CHUNKS, 8)),
            DMA((CHUNKS, 32)),
            DMA((CHUNKS, 32)),
            DMA((8,)),
            DMA((8,)),
            DMA((32,)),
            DMA((32,)),
        ],
        collective_id=0,
    )(model_image.reshape(2, 4, 8, 32, 256), word_row)
    a = a.reshape(8, 4, 2, 32, 256)
    tiles = call(
        gather_kernel,
        f32(256, 128),
        [SMEM] + in_vmem(6),
        [
            pltpu.VMEM((256, 2, 8, 128), F32),
            pltpu.VMEM((2, 256, 2048), BF16),
            pltpu.VMEM((2, 2048, 128), F32),
            pltpu.VMEM((2, 2048, 128), F32),
            pltpu.VMEM((2, 2048, 8, 128), F32),
            pltpu.VMEM((4, 256, 128), F32),
            pltpu.VMEM((8, 256, 128), F32),
            pltpu.VMEM((8, 256, 128), F32),
            pltpu.VMEM((256, 128), F32),
            DMA((8,)),
            DMA((8,)),
            DMA((32,)),
            DMA((32,)),
        ],
        collective_id=3,
    )(words, a, tw, rows, columns, screens, spread)
    vis, every = call(
        subgrid_kernel,
        (f32(32, 128), f32(8, 256, 128)),
        in_vmem(9),
        [pltpu.VMEM((256, 128), F32), DMA((32,)), DMA((32,)), DMA((4, 4)), DMA((4, 4)), DMA((3, 4)), DMA((3, 4))],
        collective_id=1,
    )(
        tiles, right, left, wa, wb, pa, pb, vis_observed.reshape(32, 128), live
    )
    every = every.reshape(2048, 128)
    spots = call(
        scatter_kernel,
        f32(8, 4, 2, 32, 256),
        [SMEM] + in_vmem(6),
        [
            pltpu.VMEM((256, 2, 8, 128), F32),
            pltpu.VMEM((2, 256, 2048), BF16),
            pltpu.VMEM((2, 2048, 128), F32),
            pltpu.VMEM((4, 2048, 128), F32),
            pltpu.VMEM((2, 2048, 8, 128), F32),
            pltpu.VMEM((2, 2048, 8, 128), F32),
        ],
    )(words, every, tw, rows, columns, screens, spread)
    image = call(
        backward_kernel,
        f32(2, 4, 8, 32, 256),
        [ANY],
        [
            pltpu.VMEM((32, 2, 32, 256), F32),
            pltpu.VMEM((8, 2, 4, 32, 256), F32),
            DMA,
            DMA((CHUNKS,)),
            DMA((CHUNKS, 32)),
            DMA((CHUNKS, 32)),
            DMA((CHUNKS, 8)),
            DMA((CHUNKS, 8)),
        ],
        collective_id=2,
        out_specs=ANY,
    )(spots.reshape(32, 2, 32, 256)).reshape(2, 1024, 256)
    return image, vis.reshape(16, 2, 128)


def solution(mesh):
    torus = Mesh(mesh.devices.reshape(mesh.shape["slab"], 8, 4), SLAB_BL)
    in_specs = (
        P(None, "slab", BL),
        P(SLAB_BL, None, None),
        P(SLAB_BL, None, None),
        P(SLAB_BL),
        P(SLAB_BL, None),
        P(SLAB_BL),
        P(SLAB_BL),
    )
    out_specs = (P(None, "slab", BL), P(SLAB_BL, None, None))
    return jax.shard_map(per_device, mesh=torus, in_specs=in_specs, out_specs=out_specs, check_vma=False)
```

```python
import functools
import math

import jax
import jax.numpy as jnp
import numpy as np
from jax import lax
from jax.experimental import pallas as pl
from jax.experimental.pallas import tpu as pltpu
from jax.sharding import Mesh
from jax.sharding import PartitionSpec as P

N = 8192
SUB = 32
BL = ("bl_0", "bl_1")
SLAB_BL = ("slab", "bl_0", "bl_1")
PLANE = ("slab", "bl_1")
W_STEP = 0.1
F32 = jnp.float32
BF16 = jnp.bfloat16
HIGHEST = lax.Precision.HIGHEST
MESH = pl.DeviceIdType.MESH
ANY = pl.BlockSpec(memory_space=pl.ANY)
DMA = pltpu.SemaphoreType.DMA


def unit(numerator, modulus):
    angle = 2.0 * np.pi * (numerator % modulus) / modulus
    return np.cos(angle), np.sin(angle)


def halves(value):
    high = value.astype(BF16)
    return high, (value - high.astype(F32)).astype(BF16)


def np_halves(value):
    value = np.asarray(value, np.float32)
    high = value.astype(BF16)
    return np.stack([high, (value - high.astype(np.float32)).astype(BF16)])


def row_tables():
    index = np.arange(256)
    cos, sin = unit(np.outer(index, index), 256)
    return np.concatenate([np_halves(cos), np_halves(sin)])


def column_tables():
    a = np.arange(128)[:, None]
    v = np.arange(1024)[None, :]
    cos, sin = unit(a * v, 1024)
    return np.concatenate([np_halves(cos), np_halves(sin)])


def screen_tables():
    b = np.arange(8)[:, None]
    v = np.arange(N)[None, :]
    cos, sin = unit(b * v, N)
    both = np.stack([cos, -sin]).reshape(2, 8, 64, 128)
    return both.transpose(2, 0, 1, 3).astype(np.float32)


def dot(left, right):
    return jnp.dot(left, right, preferred_element_type=F32)


def dot_t(left, right):
    return lax.dot_general(left, right, (((1,), (1,)), ((), ())), preferred_element_type=F32)


def dot3(left, right, product=dot):
    return product(left[0], right[0]) + (product(left[0], right[1]) + product(left[1], right[0]))


def dft4(values, sign):
    (ar, ai), (br, bi), (cr, ci), (dr, di) = values
    pr, pi, mr, mi = ar + cr, ai + ci, ar - cr, ai - ci
    qr, qi, nr, ni = br + dr, bi + di, br - dr, bi - di
    return [
        (pr + qr, pi + qi),
        (mr - sign * ni, mi + sign * nr),
        (pr - qr, pi - qi),
        (mr + sign * ni, mi - sign * nr),
    ]


def turn(value, numerator, modulus, sign):
    cos, sin = math.cos(2 * math.pi * numerator / modulus), sign * math.sin(2 * math.pi * numerator / modulus)
    if numerator % modulus == 0:
        return value
    re, im = value
    return (re * cos - im * sin, re * sin + im * cos)


def dft8(values, sign):
    even, odd = dft4(values[0::2], sign), dft4(values[1::2], sign)
    out = [None] * 8
    for k in range(4):
        tr, ti = turn(odd[k], k, 8, sign)
        out[k] = (even[k][0] + tr, even[k][1] + ti)
        out[k + 4] = (even[k][0] - tr, even[k][1] - ti)
    return out


def butterfly(v_ref, w_ref, c):
    def tile(step, carry):
        rows = pl.ds(pl.multiple_of(32 // CHUNKS * c + step // 2 * 8, 8), 8)
        lanes = pl.ds(pl.multiple_of(step % 2 * 128, 128), 128)
        mid = []
        for b in range(4):
            column = dft8([(v_ref[s, 0, b, rows, lanes], v_ref[s, 1, b, rows, lanes]) for s in range(8)], -1.0)
            mid.append([turn(column[i0], i0 * b, 32, -1.0) for i0 in range(8)])
        for i0 in range(8):
            done = dft4([mid[b][i0] for b in range(4)], -1.0)
            for i1 in range(4):
                w_ref[i0 + 8 * i1, 0, rows, lanes] = done[i1][0]
                w_ref[i0 + 8 * i1, 1, rows, lanes] = done[i1][1]
        return carry

    lax.fori_loop(0, 8 // CHUNKS, tile, 0)


def unbutterfly(w_ref, v_ref, c):
    def tile(step, carry):
        rows = pl.ds(pl.multiple_of(32 // CHUNKS * c + step // 2 * 8, 8), 8)
        lanes = pl.ds(pl.multiple_of(step % 2 * 128, 128), 128)
        mid = []
        for i0 in range(8):
            column = dft4([(w_ref[i0 + 8 * i1, 0, rows, lanes], w_ref[i0 + 8 * i1, 1, rows, lanes]) for i1 in range(4)], 1.0)
            mid.append([turn(column[b], i0 * b, 32, 1.0) for b in range(4)])
        for b in range(4):
            done = dft8([mid[i0][b] for i0 in range(8)], 1.0)
            for s in range(8):
                v_ref[s, 0, b, rows, lanes] = done[s][0]
                v_ref[s, 1, b, rows, lanes] = done[s][1]
        return carry

    lax.fori_loop(0, 8 // CHUNKS, tile, 0)


def remote(src, dst, send, recv, device):
    return pltpu.make_async_remote_copy(
        src_ref=src, dst_ref=dst, send_sem=send, recv_sem=recv, device_id=device, device_id_type=MESH
    )


def each(count, body):
    def step(at, carry):
        body(at)
        return carry

    lax.fori_loop(1, count, step, 0)


def place_of(peer, z):
    return (peer // 4, z, peer % 4)


def greet(plane, along_z):
    slab, z, x = (lax.axis_index(a) for a in SLAB_BL)
    own = slab * 4 + x
    barrier = pltpu.get_barrier_semaphore()
    if plane:
        each(32, lambda d: pl.semaphore_signal(barrier, inc=1, device_id=place_of((own + d) % 32, z), device_id_type=MESH))
    if along_z:
        each(8, lambda d: pl.semaphore_signal(barrier, inc=1, device_id=(slab, (z + d) % 8, x), device_id_type=MESH))
    pl.semaphore_wait(barrier, 31 * plane + 7 * along_z)
    return slab, z, x, own


CHUNKS = 2
STEP8 = 3
STEP32 = 13


def chunk(c):
    return pl.ds(32 // CHUNKS * c, 32 // CHUNKS)


def device_tables(slab, z, own, coord_ref, plane_ref, count_ref, pa_ref, pb_ref, wa_ref, wb_ref, live_ref, tw_ref, f_ref):
    def iota(shape, dim):
        return lax.broadcasted_iota(jnp.int32, shape, dim)

    offsets = (iota((SUB, 128), 0) - SUB // 2).astype(F32)

    def subgrid_phases(g, carry):
        for at, out_ref in enumerate((pa_ref, pb_ref)):
            along = (-2.0 * math.pi / SUB) * coord_ref[pl.ds(2 * g + at, 1), :] * offsets
            out_ref[0, g], out_ref[1, g] = jnp.cos(along), jnp.sin(along)
        live_ref[pl.ds(g, 1), :] = jnp.where(iota((1, 128), 1) < count_ref[g], 1.0, 0.0)
        return carry

    lax.fori_loop(0, 16, subgrid_phases, 0)
    lane = iota((SUB, 128), 1)
    across = (lane % SUB - SUB // 2).astype(F32)
    radius = (offsets * offsets + across * across) * (1.0 / (SUB // 2) ** 2)

    def screens(k, carry):
        plane = jnp.where(lane < 64, plane_ref[k].astype(F32), plane_ref[k + 8].astype(F32))
        phase = -W_STEP * plane * radius
        wa_ref[k], wb_ref[k] = jnp.cos(phase), jnp.sin(phase)
        return carry

    lax.fori_loop(0, 8, screens, 0)
    angle = (2.0 * math.pi / N) * (own * iota((256, 128), 0)).astype(F32)
    tw_ref[0], tw_ref[1] = jnp.cos(angle), -jnp.sin(angle)
    source, target = iota((128, 512), 0), iota((128, 512), 1)
    same = (source // 64 == target // 256) & (source % 32 == target % 32)
    part, n_part = source // 32 % 2, target // 128 % 2
    shift = (2.0 * math.pi / 8.0) * (target % 32 * z % 8).astype(F32)
    cos, sin = jnp.cos(shift) * (1.0 / N), jnp.sin(shift) * (1.0 / N)
    value = jnp.where(part == n_part, cos, jnp.where(part == 0, sin, -sin))
    f_ref[0], f_ref[1] = halves(jnp.where(same, value, 0.0))


def forward_kernel(
    slot_ref, group_ref, plane_ref, count_ref, image_ref, coord_ref,
    a_ref, idx_ref, pa_ref, pb_ref, wa_ref, wb_ref, live_ref, tw_ref, f_ref,
    word_ref, v_ref, w_ref, zrow_ref, row_ref, local, send1, recv1, send2, recv2, sendz, recvz, sendi, recvi,
):
    slab, z, x, own = greet(True, True)

    def word_copy(d):
        peer = (z + d) % 8
        return remote(word_ref, zrow_ref.at[z], sendz.at[d], recvz.at[z], (slab, peer, x))

    def slab_copy(c, d):
        peer = (slab + STEP8 * d) % 8
        return remote(image_ref.at[:, :, peer, chunk(c)], v_ref.at[slab, :, :, chunk(c)], send1.at[c, d], recv1.at[c, slab], (peer, z, x))

    def slab_wait(c, d):
        peer = (slab + STEP8 * d) % 8
        remote(image_ref.at[:, :, peer, chunk(c)], v_ref.at[peer, :, :, chunk(c)], send1.at[c, d], recv1.at[c, peer], (peer, z, x)).wait_recv()

    def plane_copy(c, d):
        peer = (own + STEP32 * d) % 32
        return remote(w_ref.at[peer, :, chunk(c)], a_ref.at[own, :, chunk(c)], send2.at[c, d], recv2.at[c, own], place_of(peer, z))

    def plane_wait(c, d):
        peer = (own + STEP32 * d) % 32
        remote(w_ref.at[peer, :, chunk(c)], a_ref.at[peer, :, chunk(c)], send2.at[c, d], recv2.at[c, peer], place_of(peer, z)).wait_recv()

    def row_copy(d):
        return remote(row_ref, idx_ref.at[own], sendi.at[d], recvi.at[own], place_of((own + d) % 32, z))

    lane = lax.broadcasted_iota(jnp.int32, (1, 128), 1)
    words = jnp.zeros((1, 128), jnp.int32)
    for k in range(16):
        tv = 32 * slab + group_ref[k]
        word = slot_ref[k] + 256 * ((tv >> 2) & 7) + 2048 * tv
        words = jnp.where(lane == 16 * z + k, word, words)
    word_ref[...] = words
    mine = pltpu.make_async_copy(image_ref.at[:, :, slab], v_ref.at[slab], local)
    mine.start()
    for c in range(CHUNKS):
        each(8, lambda d: slab_copy(c, d).start())
    each(8, lambda d: word_copy(d).start())
    device_tables(slab, z, own, coord_ref, plane_ref, count_ref, pa_ref, pb_ref, wa_ref, wb_ref, live_ref, tw_ref, f_ref)

    def word_wait(d):
        peer = (z + d) % 8
        remote(word_ref, zrow_ref.at[peer], sendz.at[d], recvz.at[peer], (slab, peer, x)).wait_recv()

    each(8, word_wait)
    zrow_ref[z] = word_ref[...]
    row = zrow_ref[0]
    for at in range(1, 8):
        row = row + zrow_ref[at]
    row_ref[...] = row
    idx_ref[own] = row
    mine.wait()
    for c in range(CHUNKS):
        each(8, lambda d: slab_wait(c, d))
        if c == 0:
            each(32, lambda d: row_copy(d).start())
        butterfly(v_ref, w_ref, c)
        each(32, lambda d: plane_copy(c, d).start())
        a_ref[own, :, chunk(c)] = w_ref[own, :, chunk(c)]

    def row_wait(d):
        peer = (own + STEP32 * d) % 32
        remote(row_ref, idx_ref.at[peer], sendi.at[d], recvi.at[peer], place_of(peer, z)).wait_recv()

    each(32, row_wait)
    for c in range(CHUNKS):
        each(32, lambda d: plane_wait(c, d))
    each(8, lambda d: word_copy(d).wait_send())
    each(32, lambda d: row_copy(d).wait_send())
    for c in range(CHUNKS):
        each(8, lambda d: slab_copy(c, d).wait_send())
        each(32, lambda d: plane_copy(c, d).wait_send())


def backward_kernel(spot_ref, out_ref, w_ref, v_ref, local, keep, send1, recv1, send2, recv2):
    slab, z, x, own = greet(True, False)

    def plane_copy(c, d):
        peer = (own + STEP32 * d) % 32
        return remote(spot_ref.at[peer, :, chunk(c)], w_ref.at[own, :, chunk(c)], send1.at[c, d], recv1.at[c, own], place_of(peer, z))

    def plane_wait(c, d):
        peer = (own + STEP32 * d) % 32
        remote(spot_ref.at[peer, :, chunk(c)], w_ref.at[peer, :, chunk(c)], send1.at[c, d], recv1.at[c, peer], place_of(peer, z)).wait_recv()

    def slab_copy(c, d):
        peer = (slab + STEP8 * d) % 8
        return remote(v_ref.at[peer, :, :, chunk(c)], out_ref.at[slab, :, :, chunk(c)], send2.at[c, d], recv2.at[c, slab], (peer, z, x))

    def slab_wait(c, d):
        peer = (slab + STEP8 * d) % 8
        remote(v_ref.at[peer, :, :, chunk(c)], out_ref.at[peer, :, :, chunk(c)], send2.at[c, d], recv2.at[c, peer], (peer, z, x)).wait_recv()

    mine = pltpu.make_async_copy(spot_ref.at[own], w_ref.at[own], local)
    mine.start()
    for c in range(CHUNKS):
        each(32, lambda d: plane_copy(c, d).start())
    mine.wait()
    kept = []
    for c in range(CHUNKS):
        each(32, lambda d: plane_wait(c, d))
        unbutterfly(w_ref, v_ref, c)
        each(8, lambda d: slab_copy(c, d).start())
        copy = pltpu.make_async_copy(v_ref.at[slab, :, :, chunk(c)], out_ref.at[slab, :, :, chunk(c)], keep.at[c])
        copy.start()
        kept.append(copy)
    for c in range(CHUNKS):
        each(8, lambda d: slab_wait(c, d))
        kept[c].wait()
    for c in range(CHUNKS):
        each(32, lambda d: plane_copy(c, d).wait_send())
        each(8, lambda d: slab_copy(c, d).wait_send())


def placing(x):
    c0 = lax.broadcasted_iota(jnp.int32, (256, 1024), 0)
    n = lax.broadcasted_iota(jnp.int32, (256, 1024), 1)
    hit = (c0 == 8 * (n & 31) + (n >> 7)) & (((n >> 5) & 3) == x)
    return jnp.where(hit, 1.0, 0.0).astype(BF16)


def spread_screens(w4_ref, w_ref):
    group = lax.broadcasted_iota(jnp.int32, (8, 128), 1) >> 5

    def expand(q, carry):
        for m in range(4):
            mask = group == m
            w_ref[4 * q + m, 0] = jnp.where(mask, w4_ref[q, 0], 0.0)
            w_ref[4 * q + m, 1] = jnp.where(mask, w4_ref[q, 1], 0.0)
        return carry

    lax.fori_loop(0, 64, expand, 0)


def fill_columns(m1_ref, full_ref):
    for h in range(2):
        cos, sin = m1_ref[h], m1_ref[2 + h]
        full_ref[h, 0:128, 0:1024] = cos
        full_ref[h, 0:128, 1024:2048] = -sin
        full_ref[h, 128:256, 0:1024] = sin
        full_ref[h, 128:256, 1024:2048] = cos


def row_sums(values):
    at = lax.broadcasted_iota(jnp.int32, (8, 128), 0)
    quads = []
    for r in range(4):
        first, second = values[r], values[r + 4]
        quads.append(jnp.where(at < 4, first, second) + pltpu.roll(jnp.where(at < 4, second, first), 4, 0))
    pairs = []
    for r in range(2):
        first, second = quads[r] + pltpu.roll(quads[r], 6, 0), quads[r + 2] + pltpu.roll(quads[r + 2], 2, 0)
        pairs.append(jnp.where(at & 2 == 0, first, second))
    first, second = pairs[0] + pltpu.roll(pairs[0], 7, 0), pairs[1] + pltpu.roll(pairs[1], 1, 0)
    return jnp.where(at & 1 == 0, first, second)


def gather_kernel(
    idx_ref, a_ref, tw_ref, m_ref, m1_ref, w4_ref, f_ref, out_ref,
    w_ref, full_ref, high_ref, low_ref, z_ref, s_ref, part_ref, right_ref, left_ref, sum_ref, sendr, recvr, sendl, recvl, sendp, recvp,
):
    slab, z, x, own = greet(True, True)
    spread_screens(w4_ref, w_ref)
    fill_columns(m1_ref, full_ref)
    cos, sin = (m_ref[0], m_ref[1]), (m_ref[2], m_ref[3])
    twr = jnp.concatenate([tw_ref[0]] * 2, axis=1)
    twi = jnp.concatenate([tw_ref[1]] * 2, axis=1)
    total = [None] * 4
    for xx in range(4):
        ar = a_ref[:, xx, 0].reshape(256, 256)
        ai = a_ref[:, xx, 1].reshape(256, 256)
        br, bi = halves(ar * twr - ai * twi), halves(ar * twi + ai * twr)
        ur = dot3(cos, br) + dot3(sin, bi)
        ui = dot3(cos, bi) - dot3(sin, br)
        place = placing(xx)
        for at, piece in enumerate(halves(ur) + halves(ui)):
            part = dot(piece, place)
            total[at] = part if total[at] is None else total[at] + part
    for b in range(8):
        cut = slice(128 * b, 128 * b + 128)
        rows = pl.ds(b, 256, stride=8)
        for part in range(2):
            high_ref[part, rows, :] = total[2 * part][:, cut]
            low_ref[part, rows, :] = total[2 * part + 1][:, cut]

    def stage(step, carry):
        block, part = step // 4, step % 4
        rows = pl.ds(pl.multiple_of(part * 512, 512), 512)
        lanes = pl.ds(pl.multiple_of(block * 256, 256), 256)
        left = tuple(jnp.concatenate([ref[0, rows, :], ref[1, rows, :]], axis=1).astype(BF16) for ref in (high_ref, low_ref))
        right = (full_ref[0, :, lanes], full_ref[1, :, lanes])
        res = dot3(left, right)
        z_ref[block // 4, pl.ds(pl.multiple_of(block % 4 * 512 + part * 64, 64), 64)] = res[:, 0:128].reshape(64, 8, 128)
        z_ref[block // 4, pl.ds(pl.multiple_of(block % 4 * 512 + 256 + part * 64, 64), 64)] = res[:, 128:256].reshape(64, 8, 128)
        return carry

    lax.fori_loop(0, 32, stage, 0)

    def collect(zc):
        def some(step, carry):
            for d in (2 * step, 2 * step + 1):
                for half in range(2):
                    res, ims = [], []
                    for k in range(8):
                        word = idx_ref[d, 0, zc * 16 + half * 8 + k]
                        spot, tv = word & 2047, word >> 11
                        zr, zi = z_ref[0, spot], z_ref[1, spot]
                        wr, wi = w_ref[tv, 0], w_ref[tv, 1]
                        res.append(zr * wr - zi * wi)
                        ims.append(zr * wi + zi * wr)
                    rows = pl.ds(pl.multiple_of(d * 8, 8), 8)
                    s_ref[2 * half, rows, :] = row_sums(res)
                    s_ref[2 * half + 1, rows, :] = row_sums(ims)
            return carry

        lax.fori_loop(0, 16, some, 0)
        sums = jnp.concatenate([s_ref[at] for at in range(4)], axis=1)
        part_ref[zc] = dot3(halves(sums), (f_ref[0], f_ref[1]), dot_t)

    def half_of(ref, u):
        return ref.at[pl.ds(128 * u, 128)]

    def right_copy(h, u):
        src, dst = half_of(part_ref.at[(z + 4 - h) % 8], u), half_of(right_ref.at[h], u)
        return remote(src, dst, sendr.at[h, u], recvr.at[h, u], (slab, (z + 1) % 8, x))

    def left_copy(h, u):
        src, dst = half_of(part_ref.at[(z + 5 + h) % 8], u), half_of(left_ref.at[h], u)
        return remote(src, dst, sendl.at[h, u], recvl.at[h, u], (slab, (z + 7) % 8, x))

    def pass_on(zc, h, copy, held_ref):
        for u in range(2):
            rows = pl.ds(128 * u, 128)

            @pl.when(h > 0)
            def _():
                copy(jnp.maximum(h - 1, 0), u).wait_recv()
                part_ref[zc, rows, :] += held_ref[jnp.maximum(h - 1, 0), rows, :]

            copy(h, u).start()

    def outward(step, carry):
        h, odd = step // 2, step % 2
        zc = (z + (1 - odd) * (4 - h) + odd * (5 + h)) % 8
        collect(zc)

        @pl.when(odd == 0)
        def _():
            pass_on(zc, h, right_copy, right_ref)

        @pl.when((odd == 1) & (step < 7))
        def _():
            pass_on(zc, h, left_copy, left_ref)

        return carry

    lax.fori_loop(0, 8, outward, 0)
    for u in range(2):
        left_copy(2, u).wait_recv()
        right_copy(3, u).wait_recv()
    total = part_ref[z] + (right_ref[3] + left_ref[2])
    sum_ref[...] = total

    def block(d):
        return pl.ds(pl.multiple_of(8 * d, 8), 8)

    def plane_copy(d):
        peer = (own + STEP32 * d) % 32
        return remote(sum_ref.at[block(peer)], out_ref.at[block(own)], sendp.at[d], recvp.at[own], place_of(peer, z))

    def plane_wait(d):
        peer = (own + STEP32 * d) % 32
        remote(sum_ref.at[block(peer)], out_ref.at[block(peer)], sendp.at[d], recvp.at[peer], place_of(peer, z)).wait_recv()

    each(32, lambda d: plane_copy(d).start())
    out_ref[block(own), :] = sum_ref[block(own), :]
    each(32, plane_wait)
    for u in range(2):
        for h in range(4):
            right_copy(h, u).wait_send()
            if h < 3:
                left_copy(h, u).wait_send()
    each(32, lambda d: plane_copy(d).wait_send())


def scatter_kernel(idx_ref, c_ref, tw_ref, m_ref, m1_ref, w4_ref, f_ref, out_ref, w_ref, full_ref, l_ref, crep_ref, z0_ref, z1_ref):
    spread_screens(w4_ref, w_ref)
    fill_columns(m1_ref, full_ref)
    spread = dot3(halves(c_ref[...]), (f_ref[0], f_ref[1]))
    for at in range(4):
        crep_ref[at] = spread[:, 128 * at : 128 * at + 128]

    def clear(step, carry):
        spots = pl.ds(pl.multiple_of(step * 128, 128), 128)
        zero = jnp.zeros((2, 128, 8, 128), F32)
        z0_ref[:, spots] = zero
        z1_ref[:, spots] = zero
        return carry

    lax.fori_loop(0, 16, clear, 0)

    def add(it, carry):
        for k in range(16):
            z_ref = (z0_ref, z1_ref)[k % 2]
            half, row = k // 8, k % 8
            word = idx_ref[it % 32, 0, it // 32 * 16 + k]
            spot, tv = word & 2047, word >> 11
            cr = jnp.broadcast_to(crep_ref[2 * half, pl.ds(it * 8 + row, 1), :], (8, 128))
            ci = jnp.broadcast_to(crep_ref[2 * half + 1, pl.ds(it * 8 + row, 1), :], (8, 128))
            wr, wi = w_ref[tv, 0], w_ref[tv, 1]
            z_ref[0, spot] += cr * wr + ci * wi
            z_ref[1, spot] += ci * wr - cr * wi
        return carry

    lax.fori_loop(0, 256, add, 0)

    def stage(step, carry):
        res = None
        for block in range(8):
            lanes = slice(256 * block, 256 * block + 256)
            spots = [pl.ds(pl.multiple_of(t % 8 * 256 + step * 32, 32), 32) for t in (2 * block, 2 * block + 1)]
            parts = [(z0_ref[block // 4, at] + z1_ref[block // 4, at]).reshape(256, 128) for at in spots]
            left = halves(jnp.concatenate(parts, axis=1))
            part = dot3(left, (full_ref[0, :, lanes], full_ref[1, :, lanes]), dot_t)
            res = part if res is None else res + part
        rows = pl.ds(pl.multiple_of(step * 256, 256), 256)
        l_ref[0, rows, :], l_ref[1, rows, :] = res[:, 0:128], res[:, 128:256]
        return carry

    lax.fori_loop(0, 8, stage, 0)

    wide = []
    for at in range(2):
        wide += halves(jnp.concatenate([l_ref[at, pl.ds(b, 256, stride=8), :] for b in range(8)], axis=1))
    cos, sin = (m_ref[0], m_ref[1]), (m_ref[2], m_ref[3])
    twr = jnp.concatenate([tw_ref[0]] * 2, axis=1)
    twi = jnp.concatenate([tw_ref[1]] * 2, axis=1)
    for x in range(4):
        place = placing(x)
        pieces = [dot_t(piece, place).astype(BF16) for piece in wide]
        ur, ui = (pieces[0], pieces[1]), (pieces[2], pieces[3])
        ar = dot3(cos, ur) - dot3(sin, ui)
        ai = dot3(cos, ui) + dot3(sin, ur)
        out_ref[:, x, 0] = (ar * twr + ai * twi).reshape(8, 32, 256)
        out_ref[:, x, 1] = (ai * twr - ar * twi).reshape(8, 32, 256)


def hdot(left, right):
    return jnp.dot(left, right, preferred_element_type=F32, precision=HIGHEST)


def hdot_t(left, right):
    return lax.dot_general(left, right, (((1,), (1,)), ((), ())), preferred_element_type=F32, precision=HIGHEST)


def subgrid_kernel(t_ref, right_ref, left_ref, wa_ref, wb_ref, pa_ref, pb_ref, obs_ref, live_ref, vis_ref, g_ref, out_ref, send1, recv1, sendr, recvr, sendl, recvl):
    slab, z, x, own = greet(True, True)
    tiles = jnp.concatenate([t_ref[pl.ds(k, 32, stride=8), :] for k in range(8)], axis=0)
    both = hdot(tiles, right_ref[...])
    rows = []
    for k in range(8):
        cut = slice(32 * k, 32 * k + 32)
        y, iy = both[cut, 0:128], both[cut, 128:256]
        column = jnp.concatenate([jnp.concatenate([y, iy], axis=1), jnp.concatenate([iy, -y], axis=1)], axis=0)
        s_both = hdot(left_ref[0], column)
        s, i_s = s_both[:, 0:128], s_both[:, 128:256]
        wa, wb = wa_ref[k], wb_ref[k]
        weighted = wa * s + wb * i_s
        found, i_found = [], []
        for half in range(2):
            at = k + 8 * half
            ar, ai = pa_ref[0, at], pa_ref[1, at]
            br, bi = pb_ref[0, at], pb_ref[1, at]
            phase = jnp.concatenate([jnp.concatenate([br, bi], axis=1), jnp.concatenate([-bi, br], axis=1)], axis=0)
            part = hdot(weighted[:, 64 * half : 64 * half + 64], phase)
            pr, pi = part[:, 0:128], part[:, 128:256]
            live = live_ref[pl.ds(at, 1), :]
            rr = (obs_ref[pl.ds(2 * at, 1), :] - jnp.sum(ar * pr - ai * pi, axis=0, keepdims=True)) * live
            ri = (obs_ref[pl.ds(2 * at + 1, 1), :] - jnp.sum(ar * pi + ai * pr, axis=0, keepdims=True)) * live
            vis_ref[pl.ds(2 * at, 1), :] = rr
            vis_ref[pl.ds(2 * at + 1, 1), :] = ri
            sr, si = ar * rr + ai * ri, ar * ri - ai * rr
            sent = jnp.concatenate([jnp.concatenate([sr, si], axis=1), jnp.concatenate([-si, sr], axis=1)], axis=0)
            back = hdot_t(sent, phase)
            found.append(back[0:32])
            i_found.append(back[32:64])
        c, ic = jnp.concatenate(found, axis=1), jnp.concatenate(i_found, axis=1)
        r, ir = wa * c - wb * ic, wa * ic + wb * c
        rows.append(hdot(left_ref[1], jnp.concatenate([r, ir], axis=0)))
    tile = hdot_t(jnp.concatenate(rows, axis=0), right_ref[:, 0:128])
    for k in range(8):
        out_ref[pl.ds(k, 32, stride=8), :] = tile[32 * k : 32 * k + 32]

    def block(d):
        return pl.ds(pl.multiple_of(8 * d, 8), 8)

    def plane_copy(d):
        peer = (own + STEP32 * d) % 32
        return remote(out_ref.at[block(peer)], g_ref.at[z, block(own)], send1.at[d], recv1.at[own], place_of(peer, z))

    def plane_wait(d):
        peer = (own + STEP32 * d) % 32
        remote(out_ref.at[block(peer)], g_ref.at[z, block(peer)], send1.at[d], recv1.at[peer], place_of(peer, z)).wait_recv()

    each(32, lambda d: plane_copy(d).start())
    g_ref[z, block(own), :] = out_ref[block(own), :]
    each(32, plane_wait)

    def right_copy(h, u):
        ref = g_ref.at[(z + 8 - h) % 8, pl.ds(64 * u, 64)]
        return remote(ref, ref, sendr.at[h, u], recvr.at[h, u], (slab, (z + 1) % 8, x))

    def left_copy(h, u):
        ref = g_ref.at[(z + h) % 8, pl.ds(64 * u, 64)]
        return remote(ref, ref, sendl.at[h, u], recvl.at[h, u], (slab, (z + 7) % 8, x))

    def right_wait(h, u):
        ref = g_ref.at[(z + 7 - h) % 8, pl.ds(64 * u, 64)]
        remote(ref, ref, sendr.at[h, u], recvr.at[h, u], (slab, (z + 1) % 8, x)).wait_recv()

    def left_wait(h, u):
        ref = g_ref.at[(z + 1 + h) % 8, pl.ds(64 * u, 64)]
        remote(ref, ref, sendl.at[h, u], recvl.at[h, u], (slab, (z + 7) % 8, x)).wait_recv()

    for h in range(4):
        for u in range(4):
            if h:
                right_wait(h - 1, u)
            right_copy(h, u).start()
            if h < 3:
                if h:
                    left_wait(h - 1, u)
                left_copy(h, u).start()
    for u in range(4):
        left_wait(2, u)
        right_wait(3, u)
    each(32, lambda d: plane_copy(d).wait_send())
    for u in range(4):
        for h in range(4):
            right_copy(h, u).wait_send()
            if h < 3:
                left_copy(h, u).wait_send()


def subgrid_tables():
    index = np.arange(SUB)
    cos, sin = unit(index[:, None] * (index[None, :] - SUB // 2), SUB)
    one = np.block([[cos, sin], [-sin, cos]])
    turned = np.block([[-sin, cos], [-cos, -sin]])
    zero = np.zeros_like(one)
    right = np.concatenate([np.block([[one, zero], [zero, one]]), np.block([[turned, zero], [zero, turned]])], axis=1)
    left = np.stack([np.concatenate([cos.T, sin.T], axis=1), np.concatenate([cos, -sin], axis=1)])
    return right.astype(np.float32), (left / (SUB * SUB)).astype(np.float32)


def in_vmem(count):
    return [pl.BlockSpec(memory_space=pltpu.VMEM)] * count


def call(kernel, out, specs, scratch=(), collective_id=None, out_specs=None, vmem=62):
    return pl.pallas_call(
        kernel,
        out_shape=out,
        in_specs=specs,
        out_specs=out_specs or jax.tree.map(lambda _: pl.BlockSpec(memory_space=pltpu.VMEM), out),
        scratch_shapes=list(scratch),
        compiler_params=pltpu.CompilerParams(
            vmem_limit_bytes=vmem * 1024 * 1024, collective_id=collective_id, has_side_effects=collective_id is not None
        ),
    )


def f32(*shape):
    return jax.ShapeDtypeStruct(shape, F32)


SMEM = pl.BlockSpec(memory_space=pltpu.SMEM)


def per_device(model_image, vis_coords, vis_observed, tile_slot, tile_group, w_plane, vis_count):
    rows, columns, screens = row_tables(), column_tables(), screen_tables()
    right, left = subgrid_tables()

    a, words, pa, pb, wa, wb, live, tw, spread = call(
        forward_kernel,
        (
            f32(32, 2, 32, 256),
            jax.ShapeDtypeStruct((32, 1, 128), jnp.int32),
            f32(2, 16, 32, 128),
            f32(2, 16, 32, 128),
            f32(8, 32, 128),
            f32(8, 32, 128),
            f32(16, 128),
            f32(2, 256, 128),
            jax.ShapeDtypeStruct((2, 128, 512), BF16),
        ),
        [SMEM] * 4 + [ANY] + in_vmem(1),
        [
            pltpu.VMEM((1, 128), jnp.int32),
            pltpu.VMEM((8, 2, 4, 32, 256), F32),
            pltpu.VMEM((32, 2, 32, 256), F32),
            pltpu.VMEM((8, 1, 128), jnp.int32),
            pltpu.VMEM((1, 128), jnp.int32),
            DMA,
            DMA((CHUNKS, 8)),
            DMA((CHUNKS, 8)),
            DMA((CHUNKS, 32)),
            DMA((CHUNKS, 32)),
            DMA((8,)),
            DMA((8,)),
            DMA((32,)),
            DMA((32,)),
        ],
        collective_id=0,
    )(tile_slot, tile_group[:, 0], w_plane, vis_count, model_image.reshape(2, 4, 8, 32, 256), vis_coords.reshape(32, 128))
    a = a.reshape(8, 4, 2, 32, 256)
    tiles = call(
        gather_kernel,
        f32(256, 128),
        [SMEM] + in_vmem(6),
        [
            pltpu.VMEM((256, 2, 8, 128), F32),
            pltpu.VMEM((2, 256, 2048), BF16),
            pltpu.VMEM((2, 2048, 128), F32),
            pltpu.VMEM((2, 2048, 128), F32),
            pltpu.VMEM((2, 2048, 8, 128), F32),
            pltpu.VMEM((4, 256, 128), F32),
            pltpu.VMEM((8, 256, 128), F32),
            pltpu.VMEM((4, 256, 128), F32),
            pltpu.VMEM((3, 256, 128), F32),
            pltpu.VMEM((256, 128), F32),
            DMA((4, 2)),
            DMA((4, 2)),
            DMA((3, 2)),
            DMA((3, 2)),
            DMA((32,)),
            DMA((32,)),
        ],
        collective_id=3,
    )(words, a, tw, rows, columns, screens, spread)
    vis, every = call(
        subgrid_kernel,
        (f32(32, 128), f32(8, 256, 128)),
        in_vmem(9),
        [pltpu.VMEM((256, 128), F32), DMA((32,)), DMA((32,)), DMA((4, 4)), DMA((4, 4)), DMA((3, 4)), DMA((3, 4))],
        collective_id=1,
    )(
        tiles, right, left, wa, wb, pa, pb, vis_observed.reshape(32, 128), live
    )
    every = every.reshape(2048, 128)
    spots = call(
        scatter_kernel,
        f32(8, 4, 2, 32, 256),
        [SMEM] + in_vmem(6),
        [
            pltpu.VMEM((256, 2, 8, 128), F32),
            pltpu.VMEM((2, 256, 2048), BF16),
            pltpu.VMEM((2, 2048, 128), F32),
            pltpu.VMEM((4, 2048, 128), F32),
            pltpu.VMEM((2, 2048, 8, 128), F32),
            pltpu.VMEM((2, 2048, 8, 128), F32),
        ],
    )(words, every, tw, rows, columns, screens, spread)
    image = call(
        backward_kernel,
        f32(8, 2, 4, 32, 256),
        [ANY],
        [
            pltpu.VMEM((32, 2, 32, 256), F32),
            pltpu.VMEM((8, 2, 4, 32, 256), F32),
            DMA,
            DMA((CHUNKS,)),
            DMA((CHUNKS, 32)),
            DMA((CHUNKS, 32)),
            DMA((CHUNKS, 8)),
            DMA((CHUNKS, 8)),
        ],
        collective_id=2,
        out_specs=ANY,
        vmem=16,
    )(spots.reshape(32, 2, 32, 256))
    image = image.transpose(1, 2, 0, 3, 4).reshape(2, 1024, 256)
    return image, vis.reshape(16, 2, 128)


def solution(mesh):
    torus = Mesh(mesh.devices.reshape(mesh.shape["slab"], 8, 4), SLAB_BL)
    in_specs = (
        P(None, "slab", BL),
        P(SLAB_BL, None, None),
        P(SLAB_BL, None, None),
        P(SLAB_BL),
        P(SLAB_BL, None),
        P(SLAB_BL),
        P(SLAB_BL),
    )
    out_specs = (P(None, "slab", BL), P(SLAB_BL, None, None))
    return jax.shard_map(per_device, mesh=torus, in_specs=in_specs, out_specs=out_specs, check_vma=False)
```

```python
import functools
import math

import jax
import jax.numpy as jnp
import numpy as np
from jax import lax
from jax.experimental import pallas as pl
from jax.experimental.pallas import tpu as pltpu
from jax.sharding import Mesh
from jax.sharding import PartitionSpec as P

N = 8192
SUB = 32
BL = ("bl_0", "bl_1")
SLAB_BL = ("slab", "bl_0", "bl_1")
PLANE = ("slab", "bl_1")
W_STEP = 0.1
F32 = jnp.float32
BF16 = jnp.bfloat16
HIGHEST = lax.Precision.HIGHEST
MESH = pl.DeviceIdType.MESH
ANY = pl.BlockSpec(memory_space=pl.ANY)
DMA = pltpu.SemaphoreType.DMA


def unit(numerator, modulus):
    angle = 2.0 * np.pi * (numerator % modulus) / modulus
    return np.cos(angle), np.sin(angle)


def halves(value):
    high = value.astype(BF16)
    return high, (value - high.astype(F32)).astype(BF16)


def np_halves(value):
    value = np.asarray(value, np.float32)
    high = value.astype(BF16)
    return np.stack([high, (value - high.astype(np.float32)).astype(BF16)])


def row_tables():
    index = np.arange(256)
    cos, sin = unit(np.outer(index, index), 256)
    return np.concatenate([np_halves(cos), np_halves(sin)])


def column_tables():
    a = np.arange(128)[:, None]
    v = np.arange(1024)[None, :]
    cos, sin = unit(a * v, 1024)
    return np.concatenate([np_halves(cos), np_halves(sin)])


def screen_tables():
    b = np.arange(8)[:, None]
    v = np.arange(N)[None, :]
    cos, sin = unit(b * v, N)
    both = np.stack([cos, -sin]).reshape(2, 8, 64, 128)
    return both.transpose(2, 0, 1, 3).astype(np.float32)


def dot(left, right):
    return jnp.dot(left, right, preferred_element_type=F32)


def dot_t(left, right):
    return lax.dot_general(left, right, (((1,), (1,)), ((), ())), preferred_element_type=F32)


def dot3(left, right, product=dot):
    return product(left[0], right[0]) + (product(left[0], right[1]) + product(left[1], right[0]))


def dft4(values, sign):
    (ar, ai), (br, bi), (cr, ci), (dr, di) = values
    pr, pi, mr, mi = ar + cr, ai + ci, ar - cr, ai - ci
    qr, qi, nr, ni = br + dr, bi + di, br - dr, bi - di
    return [
        (pr + qr, pi + qi),
        (mr - sign * ni, mi + sign * nr),
        (pr - qr, pi - qi),
        (mr + sign * ni, mi - sign * nr),
    ]


def turn(value, numerator, modulus, sign):
    cos, sin = math.cos(2 * math.pi * numerator / modulus), sign * math.sin(2 * math.pi * numerator / modulus)
    if numerator % modulus == 0:
        return value
    re, im = value
    return (re * cos - im * sin, re * sin + im * cos)


def dft8(values, sign):
    even, odd = dft4(values[0::2], sign), dft4(values[1::2], sign)
    out = [None] * 8
    for k in range(4):
        tr, ti = turn(odd[k], k, 8, sign)
        out[k] = (even[k][0] + tr, even[k][1] + ti)
        out[k + 4] = (even[k][0] - tr, even[k][1] - ti)
    return out


def butterfly(v_ref, w_ref, c):
    def tile(step, carry):
        rows = pl.ds(pl.multiple_of(32 // CHUNKS * c + step // 2 * 8, 8), 8)
        lanes = pl.ds(pl.multiple_of(step % 2 * 128, 128), 128)
        mid = []
        for b in range(4):
            column = dft8([(v_ref[s, 0, b, rows, lanes], v_ref[s, 1, b, rows, lanes]) for s in range(8)], -1.0)
            mid.append([turn(column[i0], i0 * b, 32, -1.0) for i0 in range(8)])
        for i0 in range(8):
            done = dft4([mid[b][i0] for b in range(4)], -1.0)
            for i1 in range(4):
                w_ref[i0 + 8 * i1, 0, rows, lanes] = done[i1][0]
                w_ref[i0 + 8 * i1, 1, rows, lanes] = done[i1][1]
        return carry

    lax.fori_loop(0, 8 // CHUNKS, tile, 0)


def unbutterfly(w_ref, v_ref, c):
    def tile(step, carry):
        rows = pl.ds(pl.multiple_of(32 // CHUNKS * c + step // 2 * 8, 8), 8)
        lanes = pl.ds(pl.multiple_of(step % 2 * 128, 128), 128)
        mid = []
        for i0 in range(8):
            column = dft4([(w_ref[i0 + 8 * i1, 0, rows, lanes], w_ref[i0 + 8 * i1, 1, rows, lanes]) for i1 in range(4)], 1.0)
            mid.append([turn(column[b], i0 * b, 32, 1.0) for b in range(4)])
        for b in range(4):
            done = dft8([mid[i0][b] for i0 in range(8)], 1.0)
            for s in range(8):
                v_ref[s, 0, b, rows, lanes] = done[s][0]
                v_ref[s, 1, b, rows, lanes] = done[s][1]
        return carry

    lax.fori_loop(0, 8 // CHUNKS, tile, 0)


def remote(src, dst, send, recv, device):
    return pltpu.make_async_remote_copy(
        src_ref=src, dst_ref=dst, send_sem=send, recv_sem=recv, device_id=device, device_id_type=MESH
    )


def each(count, body):
    def step(at, carry):
        body(at)
        return carry

    lax.fori_loop(1, count, step, 0)


def place_of(peer, z):
    return (peer // 4, z, peer % 4)


def greet(plane, along_z):
    slab, z, x = (lax.axis_index(a) for a in SLAB_BL)
    own = slab * 4 + x
    barrier = pltpu.get_barrier_semaphore()
    if plane:
        each(32, lambda d: pl.semaphore_signal(barrier, inc=1, device_id=place_of((own + d) % 32, z), device_id_type=MESH))
    if along_z:
        each(8, lambda d: pl.semaphore_signal(barrier, inc=1, device_id=(slab, (z + d) % 8, x), device_id_type=MESH))
    pl.semaphore_wait(barrier, 31 * plane + 7 * along_z)
    return slab, z, x, own


CHUNKS = 2
STEP8 = 3
STEP32 = 13


def chunk(c):
    return pl.ds(32 // CHUNKS * c, 32 // CHUNKS)


def device_tables(slab, z, own, coord_ref, plane_ref, count_ref, pa_ref, pb_ref, wa_ref, wb_ref, live_ref, tw_ref, f_ref):
    def iota(shape, dim):
        return lax.broadcasted_iota(jnp.int32, shape, dim)

    offsets = (iota((SUB, 128), 0) - SUB // 2).astype(F32)

    def subgrid_phases(g, carry):
        for at, out_ref in enumerate((pa_ref, pb_ref)):
            along = (-2.0 * math.pi / SUB) * coord_ref[pl.ds(2 * g + at, 1), :] * offsets
            out_ref[0, g], out_ref[1, g] = jnp.cos(along), jnp.sin(along)
        live_ref[pl.ds(g, 1), :] = jnp.where(iota((1, 128), 1) < count_ref[g], 1.0, 0.0)
        return carry

    lax.fori_loop(0, 16, subgrid_phases, 0)
    lane = iota((SUB, 128), 1)
    across = (lane % SUB - SUB // 2).astype(F32)
    radius = (offsets * offsets + across * across) * (1.0 / (SUB // 2) ** 2)

    def screens(k, carry):
        plane = jnp.where(lane < 64, plane_ref[k].astype(F32), plane_ref[k + 8].astype(F32))
        phase = -W_STEP * plane * radius
        wa_ref[k], wb_ref[k] = jnp.cos(phase), jnp.sin(phase)
        return carry

    lax.fori_loop(0, 8, screens, 0)
    angle = (2.0 * math.pi / N) * (own * iota((256, 128), 0)).astype(F32)
    tw_ref[0], tw_ref[1] = jnp.cos(angle), -jnp.sin(angle)
    source, target = iota((128, 512), 0), iota((128, 512), 1)
    same = (source // 64 == target // 256) & (source % 32 == target % 32)
    part, n_part = source // 32 % 2, target // 128 % 2
    shift = (2.0 * math.pi / 8.0) * (target % 32 * z % 8).astype(F32)
    cos, sin = jnp.cos(shift) * (1.0 / N), jnp.sin(shift) * (1.0 / N)
    value = jnp.where(part == n_part, cos, jnp.where(part == 0, sin, -sin))
    f_ref[0], f_ref[1] = halves(jnp.where(same, value, 0.0))


def backward_kernel(spot_ref, out_ref, w_ref, v_ref, local, keep, send1, recv1, send2, recv2):
    slab, z, x, own = greet(True, False)

    def plane_copy(c, d):
        peer = (own + STEP32 * d) % 32
        return remote(spot_ref.at[peer, :, chunk(c)], w_ref.at[own, :, chunk(c)], send1.at[c, d], recv1.at[c, own], place_of(peer, z))

    def plane_wait(c, d):
        peer = (own + STEP32 * d) % 32
        remote(spot_ref.at[peer, :, chunk(c)], w_ref.at[peer, :, chunk(c)], send1.at[c, d], recv1.at[c, peer], place_of(peer, z)).wait_recv()

    def slab_copy(c, d):
        peer = (slab + STEP8 * d) % 8
        return remote(v_ref.at[peer, :, :, chunk(c)], out_ref.at[slab, :, :, chunk(c)], send2.at[c, d], recv2.at[c, slab], (peer, z, x))

    def slab_wait(c, d):
        peer = (slab + STEP8 * d) % 8
        remote(v_ref.at[peer, :, :, chunk(c)], out_ref.at[peer, :, :, chunk(c)], send2.at[c, d], recv2.at[c, peer], (peer, z, x)).wait_recv()

    mine = pltpu.make_async_copy(spot_ref.at[own], w_ref.at[own], local)
    mine.start()
    for c in range(CHUNKS):
        each(32, lambda d: plane_copy(c, d).start())
    mine.wait()
    kept = []
    for c in range(CHUNKS):
        each(32, lambda d: plane_wait(c, d))
        unbutterfly(w_ref, v_ref, c)
        each(8, lambda d: slab_copy(c, d).start())
        copy = pltpu.make_async_copy(v_ref.at[slab, :, :, chunk(c)], out_ref.at[slab, :, :, chunk(c)], keep.at[c])
        copy.start()
        kept.append(copy)
    for c in range(CHUNKS):
        each(8, lambda d: slab_wait(c, d))
        kept[c].wait()
    for c in range(CHUNKS):
        each(32, lambda d: plane_copy(c, d).wait_send())
        each(8, lambda d: slab_copy(c, d).wait_send())


def placing(x):
    c0 = lax.broadcasted_iota(jnp.int32, (256, 1024), 0)
    n = lax.broadcasted_iota(jnp.int32, (256, 1024), 1)
    hit = (c0 == 8 * (n & 31) + (n >> 7)) & (((n >> 5) & 3) == x)
    return jnp.where(hit, 1.0, 0.0).astype(BF16)


def spread_screens(w4_ref, w_ref):
    group = lax.broadcasted_iota(jnp.int32, (8, 128), 1) >> 5

    def expand(q, carry):
        for m in range(4):
            mask = group == m
            w_ref[4 * q + m, 0] = jnp.where(mask, w4_ref[q, 0], 0.0)
            w_ref[4 * q + m, 1] = jnp.where(mask, w4_ref[q, 1], 0.0)
        return carry

    lax.fori_loop(0, 64, expand, 0)


def fill_columns(m1_ref, full_ref):
    for h in range(2):
        cos, sin = m1_ref[h], m1_ref[2 + h]
        full_ref[h, 0:128, 0:1024] = cos
        full_ref[h, 0:128, 1024:2048] = -sin
        full_ref[h, 128:256, 0:1024] = sin
        full_ref[h, 128:256, 1024:2048] = cos


def row_sums(values):
    at = lax.broadcasted_iota(jnp.int32, (8, 128), 0)
    quads = []
    for r in range(4):
        first, second = values[r], values[r + 4]
        quads.append(jnp.where(at < 4, first, second) + pltpu.roll(jnp.where(at < 4, second, first), 4, 0))
    pairs = []
    for r in range(2):
        first, second = quads[r] + pltpu.roll(quads[r], 6, 0), quads[r + 2] + pltpu.roll(quads[r + 2], 2, 0)
        pairs.append(jnp.where(at & 2 == 0, first, second))
    first, second = pairs[0] + pltpu.roll(pairs[0], 7, 0), pairs[1] + pltpu.roll(pairs[1], 1, 0)
    return jnp.where(at & 1 == 0, first, second)


def forward_kernel(
    slot_ref, group_ref, plane_ref, count_ref, image_ref, coord_ref, obs_ref, m_ref, m1_ref, w4_ref, dr_ref, dl_ref,
    vis_ref, g_ref, idx_ref, tw_ref, f_ref,
    pa_ref, pb_ref, wa_ref, wb_ref, live_ref, tiles_ref, back_ref,
    word_ref, v_ref, b_ref, zrow_ref, row_ref, a_ref, words_ref,
    w_ref, full_ref, high_ref, low_ref, z_ref, s_ref, part_ref, right_ref, left_ref, sum_ref,
    local, fetched, send1, recv1, send2, recv2, sendw, recvw, sendi, recvi, sendr, recvr, sendl, recvl, sendp, recvp,
    sendq, recvq, sendt, recvt, sendu, recvu,
):
    slab, z, x, own = greet(True, True)

    def word_copy(d):
        peer = (z + d) % 8
        return remote(word_ref, zrow_ref.at[z], sendw.at[d], recvw.at[z], (slab, peer, x))

    def slab_copy(c, d):
        peer = (slab + STEP8 * d) % 8
        return remote(image_ref.at[:, :, peer, chunk(c)], v_ref.at[slab, :, :, chunk(c)], send1.at[c, d], recv1.at[c, slab], (peer, z, x))

    def slab_wait(c, d):
        peer = (slab + STEP8 * d) % 8
        remote(image_ref.at[:, :, peer, chunk(c)], v_ref.at[peer, :, :, chunk(c)], send1.at[c, d], recv1.at[c, peer], (peer, z, x)).wait_recv()

    def row_block_copy(c, d):
        peer = (own + STEP32 * d) % 32
        return remote(b_ref.at[peer, :, chunk(c)], a_ref.at[own, :, chunk(c)], send2.at[c, d], recv2.at[c, own], place_of(peer, z))

    def row_block_wait(c, d):
        peer = (own + STEP32 * d) % 32
        remote(b_ref.at[peer, :, chunk(c)], a_ref.at[peer, :, chunk(c)], send2.at[c, d], recv2.at[c, peer], place_of(peer, z)).wait_recv()

    def row_copy(d):
        return remote(row_ref, idx_ref.at[own], sendi.at[d], recvi.at[own], place_of((own + d) % 32, z))

    lane = lax.broadcasted_iota(jnp.int32, (1, 128), 1)
    words = jnp.zeros((1, 128), jnp.int32)
    for k in range(16):
        tv = 32 * slab + group_ref[k]
        word = slot_ref[k] + 256 * ((tv >> 2) & 7) + 2048 * tv
        words = jnp.where(lane == 16 * z + k, word, words)
    word_ref[...] = words
    mine = pltpu.make_async_copy(image_ref.at[:, :, slab], v_ref.at[slab], local)
    mine.start()
    for c in range(CHUNKS):
        each(8, lambda d: slab_copy(c, d).start())
    each(8, lambda d: word_copy(d).start())
    device_tables(slab, z, own, coord_ref, plane_ref, count_ref, pa_ref, pb_ref, wa_ref, wb_ref, live_ref, tw_ref, f_ref)
    spread_screens(w4_ref, w_ref)
    fill_columns(m1_ref, full_ref)

    def word_wait(d):
        peer = (z + d) % 8
        remote(word_ref, zrow_ref.at[peer], sendw.at[d], recvw.at[peer], (slab, peer, x)).wait_recv()

    each(8, word_wait)
    zrow_ref[z] = word_ref[...]
    row = zrow_ref[0]
    for at in range(1, 8):
        row = row + zrow_ref[at]
    row_ref[...] = row
    idx_ref[own] = row
    mine.wait()
    for c in range(CHUNKS):
        each(8, lambda d: slab_wait(c, d))
        if c == 0:
            each(32, lambda d: row_copy(d).start())
        butterfly(v_ref, b_ref, c)
        each(32, lambda d: row_block_copy(c, d).start())
        a_ref[own, :, chunk(c)] = b_ref[own, :, chunk(c)]

    def row_wait(d):
        peer = (own + STEP32 * d) % 32
        remote(row_ref, idx_ref.at[peer], sendi.at[d], recvi.at[peer], place_of(peer, z)).wait_recv()

    each(32, row_wait)
    fetch = pltpu.make_async_copy(idx_ref, words_ref, fetched)
    fetch.start()
    for c in range(CHUNKS):
        each(32, lambda d: row_block_wait(c, d))

    cos, sin = (m_ref[0], m_ref[1]), (m_ref[2], m_ref[3])
    twr = jnp.concatenate([tw_ref[0]] * 2, axis=1)
    twi = jnp.concatenate([tw_ref[1]] * 2, axis=1)
    total = [None] * 4
    for xx in range(4):
        ar = jnp.concatenate([a_ref[4 * a1 + xx, 0] for a1 in range(8)], axis=0)
        ai = jnp.concatenate([a_ref[4 * a1 + xx, 1] for a1 in range(8)], axis=0)
        br, bi = halves(ar * twr - ai * twi), halves(ar * twi + ai * twr)
        ur = dot3(cos, br) + dot3(sin, bi)
        ui = dot3(cos, bi) - dot3(sin, br)
        place = placing(xx)
        for at, piece in enumerate(halves(ur) + halves(ui)):
            part = dot(piece, place)
            total[at] = part if total[at] is None else total[at] + part
    for b in range(8):
        cut = slice(128 * b, 128 * b + 128)
        rows = pl.ds(b, 256, stride=8)
        for part in range(2):
            high_ref[part, rows, :] = total[2 * part][:, cut]
            low_ref[part, rows, :] = total[2 * part + 1][:, cut]

    def stage(step, carry):
        block, part = step // 4, step % 4
        rows = pl.ds(pl.multiple_of(part * 512, 512), 512)
        lanes = pl.ds(pl.multiple_of(block * 256, 256), 256)
        left = tuple(jnp.concatenate([ref[0, rows, :], ref[1, rows, :]], axis=1).astype(BF16) for ref in (high_ref, low_ref))
        right = (full_ref[0, :, lanes], full_ref[1, :, lanes])
        res = dot3(left, right)
        z_ref[block // 4, pl.ds(pl.multiple_of(block % 4 * 512 + part * 64, 64), 64)] = res[:, 0:128].reshape(64, 8, 128)
        z_ref[block // 4, pl.ds(pl.multiple_of(block % 4 * 512 + 256 + part * 64, 64), 64)] = res[:, 128:256].reshape(64, 8, 128)
        return carry

    lax.fori_loop(0, 32, stage, 0)

    def collect(zc):
        def some(step, carry):
            for d in (2 * step, 2 * step + 1):
                for half in range(2):
                    res, ims = [], []
                    for k in range(8):
                        word = words_ref[d, 0, zc * 16 + half * 8 + k]
                        spot, tv = word & 2047, word >> 11
                        zr, zi = z_ref[0, spot], z_ref[1, spot]
                        wr, wi = w_ref[tv, 0], w_ref[tv, 1]
                        res.append(zr * wr - zi * wi)
                        ims.append(zr * wi + zi * wr)
                    rows = pl.ds(pl.multiple_of(d * 8, 8), 8)
                    s_ref[2 * half, rows, :] = row_sums(res)
                    s_ref[2 * half + 1, rows, :] = row_sums(ims)
            return carry

        lax.fori_loop(0, 16, some, 0)
        sums = jnp.concatenate([s_ref[at] for at in range(4)], axis=1)
        part_ref[zc] = dot3(halves(sums), (f_ref[0], f_ref[1]), dot_t)

    def half_of(ref, u):
        return ref.at[pl.ds(128 * u, 128)]

    def right_copy(h, u):
        src, dst = half_of(part_ref.at[(z + 4 - h) % 8], u), half_of(right_ref.at[h], u)
        return remote(src, dst, sendr.at[h, u], recvr.at[h, u], (slab, (z + 1) % 8, x))

    def left_copy(h, u):
        src, dst = half_of(part_ref.at[(z + 5 + h) % 8], u), half_of(left_ref.at[h], u)
        return remote(src, dst, sendl.at[h, u], recvl.at[h, u], (slab, (z + 7) % 8, x))

    def pass_on(zc, h, copy, held_ref):
        for u in range(2):
            rows = pl.ds(128 * u, 128)

            @pl.when(h > 0)
            def _():
                copy(jnp.maximum(h - 1, 0), u).wait_recv()
                part_ref[zc, rows, :] += held_ref[jnp.maximum(h - 1, 0), rows, :]

            copy(h, u).start()

    def outward(step, carry):
        h, odd = step // 2, step % 2
        zc = (z + (1 - odd) * (4 - h) + odd * (5 + h)) % 8
        collect(zc)

        @pl.when(odd == 0)
        def _():
            pass_on(zc, h, right_copy, right_ref)

        @pl.when((odd == 1) & (step < 7))
        def _():
            pass_on(zc, h, left_copy, left_ref)

        return carry

    fetch.wait()
    lax.fori_loop(0, 8, outward, 0)
    for u in range(2):
        left_copy(2, u).wait_recv()
        right_copy(3, u).wait_recv()
    total = part_ref[z] + (right_ref[3] + left_ref[2])
    sum_ref[...] = total

    def block(d):
        return pl.ds(pl.multiple_of(8 * d, 8), 8)

    def plane_copy(d):
        peer = (own + STEP32 * d) % 32
        return remote(sum_ref.at[block(peer)], tiles_ref.at[block(own)], sendp.at[d], recvp.at[own], place_of(peer, z))

    def plane_wait(d):
        peer = (own + STEP32 * d) % 32
        remote(sum_ref.at[block(peer)], tiles_ref.at[block(peer)], sendp.at[d], recvp.at[peer], place_of(peer, z)).wait_recv()

    each(32, lambda d: plane_copy(d).start())
    tiles_ref[block(own), :] = sum_ref[block(own), :]
    each(32, plane_wait)
    for u in range(2):
        for h in range(4):
            right_copy(h, u).wait_send()
            if h < 3:
                left_copy(h, u).wait_send()
    each(32, lambda d: plane_copy(d).wait_send())
    each(8, lambda d: word_copy(d).wait_send())
    each(32, lambda d: row_copy(d).wait_send())
    for c in range(CHUNKS):
        each(8, lambda d: slab_copy(c, d).wait_send())
        each(32, lambda d: row_block_copy(c, d).wait_send())

    tiles = jnp.concatenate([tiles_ref[pl.ds(k, 32, stride=8), :] for k in range(8)], axis=0)
    both = hdot(tiles, dr_ref[...])
    rows = []
    for k in range(8):
        cut = slice(32 * k, 32 * k + 32)
        y, iy = both[cut, 0:128], both[cut, 128:256]
        column = jnp.concatenate([jnp.concatenate([y, iy], axis=1), jnp.concatenate([iy, -y], axis=1)], axis=0)
        s_both = hdot(dl_ref[0], column)
        s, i_s = s_both[:, 0:128], s_both[:, 128:256]
        wa, wb = wa_ref[k], wb_ref[k]
        weighted = wa * s + wb * i_s
        found, i_found = [], []
        for half in range(2):
            at = k + 8 * half
            ar, ai = pa_ref[0, at], pa_ref[1, at]
            br, bi = pb_ref[0, at], pb_ref[1, at]
            phase = jnp.concatenate([jnp.concatenate([br, bi], axis=1), jnp.concatenate([-bi, br], axis=1)], axis=0)
            part = hdot(weighted[:, 64 * half : 64 * half + 64], phase)
            pr, pi = part[:, 0:128], part[:, 128:256]
            live = live_ref[pl.ds(at, 1), :]
            rr = (obs_ref[pl.ds(2 * at, 1), :] - jnp.sum(ar * pr - ai * pi, axis=0, keepdims=True)) * live
            ri = (obs_ref[pl.ds(2 * at + 1, 1), :] - jnp.sum(ar * pi + ai * pr, axis=0, keepdims=True)) * live
            vis_ref[pl.ds(2 * at, 1), :] = rr
            vis_ref[pl.ds(2 * at + 1, 1), :] = ri
            sr, si = ar * rr + ai * ri, ar * ri - ai * rr
            sent = jnp.concatenate([jnp.concatenate([sr, si], axis=1), jnp.concatenate([-si, sr], axis=1)], axis=0)
            back = hdot_t(sent, phase)
            found.append(back[0:32])
            i_found.append(back[32:64])
        c, ic = jnp.concatenate(found, axis=1), jnp.concatenate(i_found, axis=1)
        r, ir = wa * c - wb * ic, wa * ic + wb * c
        rows.append(hdot(dl_ref[1], jnp.concatenate([r, ir], axis=0)))
    tile = hdot_t(jnp.concatenate(rows, axis=0), dr_ref[:, 0:128])
    for k in range(8):
        back_ref[pl.ds(k, 32, stride=8), :] = tile[32 * k : 32 * k + 32]

    def block(d):
        return pl.ds(pl.multiple_of(8 * d, 8), 8)

    def plane_copy(d):
        peer = (own + STEP32 * d) % 32
        return remote(back_ref.at[block(peer)], g_ref.at[z, block(own)], sendq.at[d], recvq.at[own], place_of(peer, z))

    def plane_wait(d):
        peer = (own + STEP32 * d) % 32
        remote(back_ref.at[block(peer)], g_ref.at[z, block(peer)], sendq.at[d], recvq.at[peer], place_of(peer, z)).wait_recv()

    each(32, lambda d: plane_copy(d).start())
    g_ref[z, block(own), :] = back_ref[block(own), :]
    each(32, plane_wait)

    def right_copy(h, u):
        ref = g_ref.at[(z + 8 - h) % 8, pl.ds(64 * u, 64)]
        return remote(ref, ref, sendt.at[h, u], recvt.at[h, u], (slab, (z + 1) % 8, x))

    def left_copy(h, u):
        ref = g_ref.at[(z + h) % 8, pl.ds(64 * u, 64)]
        return remote(ref, ref, sendu.at[h, u], recvu.at[h, u], (slab, (z + 7) % 8, x))

    def right_wait(h, u):
        ref = g_ref.at[(z + 7 - h) % 8, pl.ds(64 * u, 64)]
        remote(ref, ref, sendt.at[h, u], recvt.at[h, u], (slab, (z + 1) % 8, x)).wait_recv()

    def left_wait(h, u):
        ref = g_ref.at[(z + 1 + h) % 8, pl.ds(64 * u, 64)]
        remote(ref, ref, sendu.at[h, u], recvu.at[h, u], (slab, (z + 7) % 8, x)).wait_recv()

    for h in range(4):
        for u in range(4):
            if h:
                right_wait(h - 1, u)
            right_copy(h, u).start()
            if h < 3:
                if h:
                    left_wait(h - 1, u)
                left_copy(h, u).start()
    for u in range(4):
        left_wait(2, u)
        right_wait(3, u)
    each(32, lambda d: plane_copy(d).wait_send())
    for u in range(4):
        for h in range(4):
            right_copy(h, u).wait_send()
            if h < 3:
                left_copy(h, u).wait_send()


def scatter_kernel(idx_ref, c_ref, tw_ref, m_ref, m1_ref, w4_ref, f_ref, out_ref, w_ref, full_ref, l_ref, crep_ref, z0_ref, z1_ref):
    spread_screens(w4_ref, w_ref)
    fill_columns(m1_ref, full_ref)
    spread = dot3(halves(c_ref[...]), (f_ref[0], f_ref[1]))
    for at in range(4):
        crep_ref[at] = spread[:, 128 * at : 128 * at + 128]

    def clear(step, carry):
        spots = pl.ds(pl.multiple_of(step * 128, 128), 128)
        zero = jnp.zeros((2, 128, 8, 128), F32)
        z0_ref[:, spots] = zero
        z1_ref[:, spots] = zero
        return carry

    lax.fori_loop(0, 16, clear, 0)

    def add(it, carry):
        for k in range(16):
            z_ref = (z0_ref, z1_ref)[k % 2]
            half, row = k // 8, k % 8
            word = idx_ref[it % 32, 0, it // 32 * 16 + k]
            spot, tv = word & 2047, word >> 11
            cr = jnp.broadcast_to(crep_ref[2 * half, pl.ds(it * 8 + row, 1), :], (8, 128))
            ci = jnp.broadcast_to(crep_ref[2 * half + 1, pl.ds(it * 8 + row, 1), :], (8, 128))
            wr, wi = w_ref[tv, 0], w_ref[tv, 1]
            z_ref[0, spot] += cr * wr + ci * wi
            z_ref[1, spot] += ci * wr - cr * wi
        return carry

    lax.fori_loop(0, 256, add, 0)

    def stage(step, carry):
        res = None
        for block in range(8):
            lanes = slice(256 * block, 256 * block + 256)
            spots = [pl.ds(pl.multiple_of(t % 8 * 256 + step * 32, 32), 32) for t in (2 * block, 2 * block + 1)]
            parts = [(z0_ref[block // 4, at] + z1_ref[block // 4, at]).reshape(256, 128) for at in spots]
            left = halves(jnp.concatenate(parts, axis=1))
            part = dot3(left, (full_ref[0, :, lanes], full_ref[1, :, lanes]), dot_t)
            res = part if res is None else res + part
        rows = pl.ds(pl.multiple_of(step * 256, 256), 256)
        l_ref[0, rows, :], l_ref[1, rows, :] = res[:, 0:128], res[:, 128:256]
        return carry

    lax.fori_loop(0, 8, stage, 0)

    wide = []
    for at in range(2):
        wide += halves(jnp.concatenate([l_ref[at, pl.ds(b, 256, stride=8), :] for b in range(8)], axis=1))
    cos, sin = (m_ref[0], m_ref[1]), (m_ref[2], m_ref[3])
    twr = jnp.concatenate([tw_ref[0]] * 2, axis=1)
    twi = jnp.concatenate([tw_ref[1]] * 2, axis=1)
    for x in range(4):
        place = placing(x)
        pieces = [dot_t(piece, place).astype(BF16) for piece in wide]
        ur, ui = (pieces[0], pieces[1]), (pieces[2], pieces[3])
        ar = dot3(cos, ur) - dot3(sin, ui)
        ai = dot3(cos, ui) + dot3(sin, ur)
        out_ref[:, x, 0] = (ar * twr + ai * twi).reshape(8, 32, 256)
        out_ref[:, x, 1] = (ai * twr - ar * twi).reshape(8, 32, 256)


def hdot(left, right):
    return jnp.dot(left, right, preferred_element_type=F32, precision=HIGHEST)


def hdot_t(left, right):
    return lax.dot_general(left, right, (((1,), (1,)), ((), ())), preferred_element_type=F32, precision=HIGHEST)


def subgrid_tables():
    index = np.arange(SUB)
    cos, sin = unit(index[:, None] * (index[None, :] - SUB // 2), SUB)
    one = np.block([[cos, sin], [-sin, cos]])
    turned = np.block([[-sin, cos], [-cos, -sin]])
    zero = np.zeros_like(one)
    right = np.concatenate([np.block([[one, zero], [zero, one]]), np.block([[turned, zero], [zero, turned]])], axis=1)
    left = np.stack([np.concatenate([cos.T, sin.T], axis=1), np.concatenate([cos, -sin], axis=1)])
    return right.astype(np.float32), (left / (SUB * SUB)).astype(np.float32)


def in_vmem(count):
    return [pl.BlockSpec(memory_space=pltpu.VMEM)] * count


def call(kernel, out, specs, scratch=(), collective_id=None, out_specs=None, vmem=62):
    return pl.pallas_call(
        kernel,
        out_shape=out,
        in_specs=specs,
        out_specs=out_specs or jax.tree.map(lambda _: pl.BlockSpec(memory_space=pltpu.VMEM), out),
        scratch_shapes=list(scratch),
        compiler_params=pltpu.CompilerParams(
            vmem_limit_bytes=vmem * 1024 * 1024, collective_id=collective_id, has_side_effects=collective_id is not None
        ),
    )


def f32(*shape):
    return jax.ShapeDtypeStruct(shape, F32)


SMEM = pl.BlockSpec(memory_space=pltpu.SMEM)


def per_device(model_image, vis_coords, vis_observed, tile_slot, tile_group, w_plane, vis_count):
    rows, columns, screens = row_tables(), column_tables(), screen_tables()
    right, left = subgrid_tables()

    vis, every, words, tw, spread = call(
        forward_kernel,
        (
            f32(32, 128),
            f32(8, 256, 128),
            jax.ShapeDtypeStruct((32, 1, 128), jnp.int32),
            f32(2, 256, 128),
            jax.ShapeDtypeStruct((2, 128, 512), BF16),
        ),
        [SMEM] * 4 + [ANY] + in_vmem(7),
        [
            pltpu.VMEM((2, 16, 32, 128), F32),
            pltpu.VMEM((2, 16, 32, 128), F32),
            pltpu.VMEM((8, 32, 128), F32),
            pltpu.VMEM((8, 32, 128), F32),
            pltpu.VMEM((16, 128), F32),
            pltpu.VMEM((256, 128), F32),
            pltpu.VMEM((256, 128), F32),
            pltpu.VMEM((1, 128), jnp.int32),
            pltpu.VMEM((8, 2, 4, 32, 256), F32),
            pltpu.VMEM((32, 2, 32, 256), F32),
            pltpu.VMEM((8, 1, 128), jnp.int32),
            pltpu.VMEM((1, 128), jnp.int32),
            pltpu.VMEM((32, 2, 32, 256), F32),
            pltpu.SMEM((32, 1, 128), jnp.int32),
            pltpu.VMEM((256, 2, 8, 128), F32),
            pltpu.VMEM((2, 256, 2048), BF16),
            pltpu.VMEM((2, 2048, 128), F32),
            pltpu.VMEM((2, 2048, 128), F32),
            pltpu.VMEM((2, 2048, 8, 128), F32),
            pltpu.VMEM((4, 256, 128), F32),
            pltpu.VMEM((8, 256, 128), F32),
            pltpu.VMEM((4, 256, 128), F32),
            pltpu.VMEM((3, 256, 128), F32),
            pltpu.VMEM((256, 128), F32),
            DMA,
            DMA,
            DMA((CHUNKS, 8)),
            DMA((CHUNKS, 8)),
            DMA((CHUNKS, 32)),
            DMA((CHUNKS, 32)),
            DMA((8,)),
            DMA((8,)),
            DMA((32,)),
            DMA((32,)),
            DMA((4, 2)),
            DMA((4, 2)),
            DMA((3, 2)),
            DMA((3, 2)),
            DMA((32,)),
            DMA((32,)),
            DMA((32,)),
            DMA((32,)),
            DMA((4, 4)),
            DMA((4, 4)),
            DMA((3, 4)),
            DMA((3, 4)),
        ],
        collective_id=0,
    )(
        tile_slot, tile_group[:, 0], w_plane, vis_count, model_image.reshape(2, 4, 8, 32, 256),
        vis_coords.reshape(32, 128), vis_observed.reshape(32, 128), rows, columns, screens, right, left,
    )
    every = every.reshape(2048, 128)
    spots = call(
        scatter_kernel,
        f32(8, 4, 2, 32, 256),
        [SMEM] + in_vmem(6),
        [
            pltpu.VMEM((256, 2, 8, 128), F32),
            pltpu.VMEM((2, 256, 2048), BF16),
            pltpu.VMEM((2, 2048, 128), F32),
            pltpu.VMEM((4, 2048, 128), F32),
            pltpu.VMEM((2, 2048, 8, 128), F32),
            pltpu.VMEM((2, 2048, 8, 128), F32),
        ],
    )(words, every, tw, rows, columns, screens, spread)
    image = call(
        backward_kernel,
        f32(8, 2, 4, 32, 256),
        [ANY],
        [
            pltpu.VMEM((32, 2, 32, 256), F32),
            pltpu.VMEM((8, 2, 4, 32, 256), F32),
            DMA,
            DMA((CHUNKS,)),
            DMA((CHUNKS, 32)),
            DMA((CHUNKS, 32)),
            DMA((CHUNKS, 8)),
            DMA((CHUNKS, 8)),
        ],
        collective_id=2,
        out_specs=ANY,
        vmem=16,
    )(spots.reshape(32, 2, 32, 256))
    image = image.transpose(1, 2, 0, 3, 4).reshape(2, 1024, 256)
    return image, vis.reshape(16, 2, 128)


def solution(mesh):
    torus = Mesh(mesh.devices.reshape(mesh.shape["slab"], 8, 4), SLAB_BL)
    in_specs = (
        P(None, "slab", BL),
        P(SLAB_BL, None, None),
        P(SLAB_BL, None, None),
        P(SLAB_BL),
        P(SLAB_BL, None),
        P(SLAB_BL),
        P(SLAB_BL),
    )
    out_specs = (P(None, "slab", BL), P(SLAB_BL, None, None))
    return jax.shard_map(per_device, mesh=torus, in_specs=in_specs, out_specs=out_specs, check_vma=False)
```

```python
import functools
import math

import jax
import jax.numpy as jnp
import numpy as np
from jax import lax
from jax.experimental import pallas as pl
from jax.experimental.pallas import tpu as pltpu
from jax.sharding import Mesh
from jax.sharding import PartitionSpec as P

N = 8192
SUB = 32
BL = ("bl_0", "bl_1")
SLAB_BL = ("slab", "bl_0", "bl_1")
PLANE = ("slab", "bl_1")
W_STEP = 0.1
F32 = jnp.float32
BF16 = jnp.bfloat16
HIGHEST = lax.Precision.HIGHEST
MESH = pl.DeviceIdType.MESH
ANY = pl.BlockSpec(memory_space=pl.ANY)
HBM = pl.BlockSpec(memory_space=pltpu.HBM)
DMA = pltpu.SemaphoreType.DMA


def unit(numerator, modulus):
    angle = 2.0 * np.pi * (numerator % modulus) / modulus
    return np.cos(angle), np.sin(angle)


def halves(value):
    high = value.astype(BF16)
    return high, (value - high.astype(F32)).astype(BF16)


def np_halves(value):
    value = np.asarray(value, np.float32)
    high = value.astype(BF16)
    return np.stack([high, (value - high.astype(np.float32)).astype(BF16)])


def row_tables():
    index = np.arange(256)
    cos, sin = unit(np.outer(index, index), 256)
    return np.concatenate([np_halves(cos), np_halves(sin)])


def column_tables():
    a = np.arange(128)[:, None]
    v = np.arange(1024)[None, :]
    cos, sin = unit(a * v, 1024)
    return np.concatenate([np_halves(cos), np_halves(sin)])


def screen_tables():
    b = np.arange(8)[:, None]
    v = np.arange(N)[None, :]
    cos, sin = unit(b * v, N)
    both = np.stack([cos, -sin]).reshape(2, 8, 64, 128)
    return both.transpose(2, 0, 1, 3).astype(np.float32)


def dot(left, right):
    return jnp.dot(left, right, preferred_element_type=F32)


def dot_t(left, right):
    return lax.dot_general(left, right, (((1,), (1,)), ((), ())), preferred_element_type=F32)


def dot3(left, right, product=dot):
    return product(left[0], right[0]) + (product(left[0], right[1]) + product(left[1], right[0]))


def dft4(values, sign):
    (ar, ai), (br, bi), (cr, ci), (dr, di) = values
    pr, pi, mr, mi = ar + cr, ai + ci, ar - cr, ai - ci
    qr, qi, nr, ni = br + dr, bi + di, br - dr, bi - di
    return [
        (pr + qr, pi + qi),
        (mr - sign * ni, mi + sign * nr),
        (pr - qr, pi - qi),
        (mr + sign * ni, mi - sign * nr),
    ]


def turn(value, numerator, modulus, sign):
    cos, sin = math.cos(2 * math.pi * numerator / modulus), sign * math.sin(2 * math.pi * numerator / modulus)
    if numerator % modulus == 0:
        return value
    re, im = value
    return (re * cos - im * sin, re * sin + im * cos)


def dft8(values, sign):
    even, odd = dft4(values[0::2], sign), dft4(values[1::2], sign)
    out = [None] * 8
    for k in range(4):
        tr, ti = turn(odd[k], k, 8, sign)
        out[k] = (even[k][0] + tr, even[k][1] + ti)
        out[k + 4] = (even[k][0] - tr, even[k][1] - ti)
    return out


def butterfly(v_ref, w_ref, c):
    def tile(step, carry):
        rows = pl.ds(pl.multiple_of(32 // CHUNKS * c + step // 2 * 8, 8), 8)
        lanes = pl.ds(pl.multiple_of(step % 2 * 128, 128), 128)
        mid = []
        for b in range(4):
            column = dft8([(v_ref[s, 0, b, rows, lanes], v_ref[s, 1, b, rows, lanes]) for s in range(8)], -1.0)
            mid.append([turn(column[i0], i0 * b, 32, -1.0) for i0 in range(8)])
        for i0 in range(8):
            done = dft4([mid[b][i0] for b in range(4)], -1.0)
            for i1 in range(4):
                w_ref[i0 + 8 * i1, 0, rows, lanes] = done[i1][0]
                w_ref[i0 + 8 * i1, 1, rows, lanes] = done[i1][1]
        return carry

    lax.fori_loop(0, 8 // CHUNKS, tile, 0)


def unbutterfly(w_ref, v_ref, c):
    def tile(step, carry):
        rows = pl.ds(pl.multiple_of(32 // CHUNKS * c + step // 2 * 8, 8), 8)
        lanes = pl.ds(pl.multiple_of(step % 2 * 128, 128), 128)
        mid = []
        for i0 in range(8):
            column = dft4([(w_ref[i0 + 8 * i1, 0, rows, lanes], w_ref[i0 + 8 * i1, 1, rows, lanes]) for i1 in range(4)], 1.0)
            mid.append([turn(column[b], i0 * b, 32, 1.0) for b in range(4)])
        for b in range(4):
            done = dft8([mid[i0][b] for i0 in range(8)], 1.0)
            for s in range(8):
                v_ref[s, 0, b, rows, lanes] = done[s][0]
                v_ref[s, 1, b, rows, lanes] = done[s][1]
        return carry

    lax.fori_loop(0, 8 // CHUNKS, tile, 0)


def remote(src, dst, send, recv, device):
    return pltpu.make_async_remote_copy(
        src_ref=src, dst_ref=dst, send_sem=send, recv_sem=recv, device_id=device, device_id_type=MESH
    )


def each(count, body):
    def step(at, carry):
        body(at)
        return carry

    lax.fori_loop(1, count, step, 0)


def place_of(peer, z):
    return (peer // 4, z, peer % 4)


def greet(plane, along_z):
    slab, z, x = (lax.axis_index(a) for a in SLAB_BL)
    own = slab * 4 + x
    barrier = pltpu.get_barrier_semaphore()
    if plane:
        each(32, lambda d: pl.semaphore_signal(barrier, inc=1, device_id=place_of((own + d) % 32, z), device_id_type=MESH))
    if along_z:
        each(8, lambda d: pl.semaphore_signal(barrier, inc=1, device_id=(slab, (z + d) % 8, x), device_id_type=MESH))
    pl.semaphore_wait(barrier, 31 * plane + 7 * along_z)
    return slab, z, x, own


CHUNKS = 2
STEP8 = 3
STEP32 = 13


def chunk(c):
    return pl.ds(32 // CHUNKS * c, 32 // CHUNKS)


def device_tables(slab, z, own, coord_ref, plane_ref, count_ref, pa_ref, pb_ref, wa_ref, wb_ref, live_ref, tw_ref, f_ref):
    def iota(shape, dim):
        return lax.broadcasted_iota(jnp.int32, shape, dim)

    offsets = (iota((SUB, 128), 0) - SUB // 2).astype(F32)

    def subgrid_phases(g, carry):
        for at, out_ref in enumerate((pa_ref, pb_ref)):
            along = (-2.0 * math.pi / SUB) * coord_ref[pl.ds(2 * g + at, 1), :] * offsets
            out_ref[0, g], out_ref[1, g] = jnp.cos(along), jnp.sin(along)
        live_ref[pl.ds(g, 1), :] = jnp.where(iota((1, 128), 1) < count_ref[g], 1.0, 0.0)
        return carry

    lax.fori_loop(0, 16, subgrid_phases, 0)
    lane = iota((SUB, 128), 1)
    across = (lane % SUB - SUB // 2).astype(F32)
    radius = (offsets * offsets + across * across) * (1.0 / (SUB // 2) ** 2)

    def screens(k, carry):
        plane = jnp.where(lane < 64, plane_ref[k].astype(F32), plane_ref[k + 8].astype(F32))
        phase = -W_STEP * plane * radius
        wa_ref[k], wb_ref[k] = jnp.cos(phase), jnp.sin(phase)
        return carry

    lax.fori_loop(0, 8, screens, 0)
    angle = (2.0 * math.pi / N) * (own * iota((256, 128), 0)).astype(F32)
    tw_ref[0], tw_ref[1] = jnp.cos(angle), -jnp.sin(angle)
    source, target = iota((128, 512), 0), iota((128, 512), 1)
    same = (source // 64 == target // 256) & (source % 32 == target % 32)
    part, n_part = source // 32 % 2, target // 128 % 2
    shift = (2.0 * math.pi / 8.0) * (target % 32 * z % 8).astype(F32)
    cos, sin = jnp.cos(shift) * (1.0 / N), jnp.sin(shift) * (1.0 / N)
    value = jnp.where(part == n_part, cos, jnp.where(part == 0, sin, -sin))
    f_ref[0], f_ref[1] = halves(jnp.where(same, value, 0.0))


def backward_kernel(spot_ref, out_ref, w_ref, v_ref, local, keep, send1, recv1, send2, recv2):
    slab, z, x, own = greet(True, False)

    def plane_copy(c, d):
        peer = (own + STEP32 * d) % 32
        return remote(spot_ref.at[peer, :, chunk(c)], w_ref.at[own, :, chunk(c)], send1.at[c, d], recv1.at[c, own], place_of(peer, z))

    def plane_wait(c, d):
        peer = (own + STEP32 * d) % 32
        remote(spot_ref.at[peer, :, chunk(c)], w_ref.at[peer, :, chunk(c)], send1.at[c, d], recv1.at[c, peer], place_of(peer, z)).wait_recv()

    def slab_copy(c, d):
        peer = (slab + STEP8 * d) % 8
        return remote(v_ref.at[peer, :, :, chunk(c)], out_ref.at[slab, :, :, chunk(c)], send2.at[c, d], recv2.at[c, slab], (peer, z, x))

    def slab_wait(c, d):
        peer = (slab + STEP8 * d) % 8
        remote(v_ref.at[peer, :, :, chunk(c)], out_ref.at[peer, :, :, chunk(c)], send2.at[c, d], recv2.at[c, peer], (peer, z, x)).wait_recv()

    mine = pltpu.make_async_copy(spot_ref.at[own], w_ref.at[own], local)
    mine.start()
    for c in range(CHUNKS):
        each(32, lambda d: plane_copy(c, d).start())
    mine.wait()
    kept = []
    for c in range(CHUNKS):
        each(32, lambda d: plane_wait(c, d))
        unbutterfly(w_ref, v_ref, c)
        each(8, lambda d: slab_copy(c, d).start())
        copy = pltpu.make_async_copy(v_ref.at[slab, :, :, chunk(c)], out_ref.at[slab, :, :, chunk(c)], keep.at[c])
        copy.start()
        kept.append(copy)
    for c in range(CHUNKS):
        each(8, lambda d: slab_wait(c, d))
        kept[c].wait()
    for c in range(CHUNKS):
        each(32, lambda d: plane_copy(c, d).wait_send())
        each(8, lambda d: slab_copy(c, d).wait_send())


def placing(x):
    c0 = lax.broadcasted_iota(jnp.int32, (256, 1024), 0)
    n = lax.broadcasted_iota(jnp.int32, (256, 1024), 1)
    hit = (c0 == 8 * (n & 31) + (n >> 7)) & (((n >> 5) & 3) == x)
    return jnp.where(hit, 1.0, 0.0).astype(BF16)


def spread_screens(w4_ref, w_ref):
    group = lax.broadcasted_iota(jnp.int32, (8, 128), 1) >> 5

    def expand(q, carry):
        for m in range(4):
            mask = group == m
            w_ref[4 * q + m, 0] = jnp.where(mask, w4_ref[q, 0], 0.0)
            w_ref[4 * q + m, 1] = jnp.where(mask, w4_ref[q, 1], 0.0)
        return carry

    lax.fori_loop(0, 64, expand, 0)


def fill_columns(m1_ref, full_ref):
    for at, h in enumerate((0, 1, 0)):
        cos, sin = m1_ref[h], m1_ref[2 + h]
        top, mid, end = 256 * at, 256 * at + 128, 256 * at + 256
        full_ref[top:mid, 0:1024] = cos
        full_ref[top:mid, 1024:2048] = -sin
        full_ref[mid:end, 0:1024] = sin
        full_ref[mid:end, 1024:2048] = cos


def row_sums(values):
    at = lax.broadcasted_iota(jnp.int32, (8, 128), 0)
    quads = []
    for r in range(4):
        first, second = values[r], values[r + 4]
        quads.append(jnp.where(at < 4, first, second) + pltpu.roll(jnp.where(at < 4, second, first), 4, 0))
    pairs = []
    for r in range(2):
        first, second = quads[r] + pltpu.roll(quads[r], 6, 0), quads[r + 2] + pltpu.roll(quads[r + 2], 2, 0)
        pairs.append(jnp.where(at & 2 == 0, first, second))
    first, second = pairs[0] + pltpu.roll(pairs[0], 7, 0), pairs[1] + pltpu.roll(pairs[1], 1, 0)
    return jnp.where(at & 1 == 0, first, second)


def forward_kernel(
    slot_ref, group_ref, plane_ref, count_ref, image_ref, coord_ref, obs_ref, dr_ref, dl_ref, m_any, m1_any, w4_any,
    vis_ref, g_ref, idx_ref, rows_ref, tw_ref, f_ref,
    pa_ref, pb_ref, wa_ref, wb_ref, live_ref, tiles_ref, back_ref,
    word_ref, v_ref, b_ref, zrow_ref, row_ref, a_ref, words_ref,
    w_ref, full_ref, high_ref, low_ref, z_ref, s_ref, part_ref, right_ref, left_ref, sum_ref,
    local, fetched, send1, recv1, send2, recv2, sendw, recvw, sendi, recvi, sendr, recvr, sendl, recvl, sendp, recvp,
    sendq, recvq, sendt, recvt, sendu, recvu, m_ref, m1_ref, w4_ref, table,
):
    slab, z, x, own = greet(True, True)

    def word_copy(d):
        peer = (z + d) % 8
        return remote(word_ref, zrow_ref.at[z], sendw.at[d], recvw.at[z], (slab, peer, x))

    def slab_copy(c, d):
        peer = (slab + STEP8 * d) % 8
        return remote(image_ref.at[:, :, peer, chunk(c)], v_ref.at[slab, :, :, chunk(c)], send1.at[c, d], recv1.at[c, slab], (peer, z, x))

    def slab_wait(c, d):
        peer = (slab + STEP8 * d) % 8
        remote(image_ref.at[:, :, peer, chunk(c)], v_ref.at[peer, :, :, chunk(c)], send1.at[c, d], recv1.at[c, peer], (peer, z, x)).wait_recv()

    def row_block_copy(c, d):
        peer = (own + STEP32 * d) % 32
        return remote(b_ref.at[peer, :, chunk(c)], a_ref.at[own, :, chunk(c)], send2.at[c, d], recv2.at[c, own], place_of(peer, z))

    def row_block_wait(c, d):
        peer = (own + STEP32 * d) % 32
        remote(b_ref.at[peer, :, chunk(c)], a_ref.at[peer, :, chunk(c)], send2.at[c, d], recv2.at[c, peer], place_of(peer, z)).wait_recv()

    def row_copy(d):
        return remote(row_ref, idx_ref.at[own], sendi.at[d], recvi.at[own], place_of((own + d) % 32, z))

    lane = lax.broadcasted_iota(jnp.int32, (1, 128), 1)
    words = jnp.zeros((1, 128), jnp.int32)
    for k in range(16):
        tv = 32 * slab + group_ref[k]
        word = slot_ref[k] + 256 * ((tv >> 2) & 7) + 2048 * tv
        words = jnp.where(lane == 16 * z + k, word, words)
    word_ref[...] = words
    mine = pltpu.make_async_copy(image_ref.at[:, :, slab], v_ref.at[slab], local)
    mine.start()
    for c in range(CHUNKS):
        each(8, lambda d: slab_copy(c, d).start())
    each(8, lambda d: word_copy(d).start())
    tables = [
        pltpu.make_async_copy(src, dst, table.at[at])
        for at, (src, dst) in enumerate(((m_any, m_ref), (m1_any, m1_ref), (w4_any, w4_ref)))
    ]
    for copy in tables:
        copy.start()
    device_tables(slab, z, own, coord_ref, plane_ref, count_ref, pa_ref, pb_ref, wa_ref, wb_ref, live_ref, tw_ref, f_ref)
    for copy in tables:
        copy.wait()
    spread_screens(w4_ref, w_ref)
    fill_columns(m1_ref, full_ref)

    def word_wait(d):
        peer = (z + d) % 8
        remote(word_ref, zrow_ref.at[peer], sendw.at[d], recvw.at[peer], (slab, peer, x)).wait_recv()

    each(8, word_wait)
    zrow_ref[z] = word_ref[...]
    row = zrow_ref[0]
    for at in range(1, 8):
        row = row + zrow_ref[at]
    row_ref[...] = row
    idx_ref[own] = row
    mine.wait()
    for c in range(CHUNKS):
        each(8, lambda d: slab_wait(c, d))
        if c == 0:
            each(32, lambda d: row_copy(d).start())
        butterfly(v_ref, b_ref, c)
        each(32, lambda d: row_block_copy(c, d).start())
        a_ref[own, :, chunk(c)] = b_ref[own, :, chunk(c)]

    def row_wait(d):
        peer = (own + STEP32 * d) % 32
        remote(row_ref, idx_ref.at[peer], sendi.at[d], recvi.at[peer], place_of(peer, z)).wait_recv()

    each(32, row_wait)
    fetch = pltpu.make_async_copy(idx_ref, words_ref, fetched)
    fetch.start()
    rows_ref[...] = 8 * (idx_ref[...] & 2047) + 262144 * (idx_ref[...] >> 11)
    for c in range(CHUNKS):
        each(32, lambda d: row_block_wait(c, d))

    cos, sin = (m_ref[0], m_ref[1]), (m_ref[2], m_ref[3])
    twr = jnp.concatenate([tw_ref[0]] * 2, axis=1)
    twi = jnp.concatenate([tw_ref[1]] * 2, axis=1)
    total = [None] * 4
    for xx in range(4):
        ar = jnp.concatenate([a_ref[4 * a1 + xx, 0] for a1 in range(8)], axis=0)
        ai = jnp.concatenate([a_ref[4 * a1 + xx, 1] for a1 in range(8)], axis=0)
        br, bi = halves(ar * twr - ai * twi), halves(ar * twi + ai * twr)
        ur = dot3(cos, br) + dot3(sin, bi)
        ui = dot3(cos, bi) - dot3(sin, br)
        place = placing(xx)
        for at, piece in enumerate(halves(ur) + halves(ui)):
            part = dot(piece, place)
            total[at] = part if total[at] is None else total[at] + part
    for b in range(8):
        cut = slice(128 * b, 128 * b + 128)
        rows = pl.ds(b, 256, stride=8)
        for part in range(2):
            high_ref[part, rows, :] = total[2 * part][:, cut]
            low_ref[part, rows, :] = total[2 * part + 1][:, cut]

    def stage(step, carry):
        block, part = step // 4, step % 4
        rows = pl.ds(pl.multiple_of(part * 512, 512), 512)
        lanes = pl.ds(pl.multiple_of(block * 256, 256), 256)
        left = tuple(jnp.concatenate([ref[0, rows, :], ref[1, rows, :]], axis=1).astype(BF16) for ref in (high_ref, low_ref))
        res = dot(jnp.concatenate([left[0], left[0], left[1]], axis=1), full_ref[:, lanes])
        z_ref[block // 4, pl.ds(pl.multiple_of(block % 4 * 512 + part * 64, 64), 64)] = res[:, 0:128].reshape(64, 8, 128)
        z_ref[block // 4, pl.ds(pl.multiple_of(block % 4 * 512 + 256 + part * 64, 64), 64)] = res[:, 128:256].reshape(64, 8, 128)
        return carry

    lax.fori_loop(0, 32, stage, 0)

    def collect(zc):
        def some(step, carry):
            for d in (2 * step, 2 * step + 1):
                for half in range(2):
                    res, ims = [], []
                    for k in range(8):
                        word = words_ref[d, 0, zc * 16 + half * 8 + k]
                        spot, tv = word & 2047, word >> 11
                        zr, zi = z_ref[0, spot], z_ref[1, spot]
                        wr, wi = w_ref[tv, 0], w_ref[tv, 1]
                        res.append(zr * wr - zi * wi)
                        ims.append(zr * wi + zi * wr)
                    rows = pl.ds(pl.multiple_of(d * 8, 8), 8)
                    s_ref[2 * half, rows, :] = row_sums(res)
                    s_ref[2 * half + 1, rows, :] = row_sums(ims)
            return carry

        lax.fori_loop(0, 16, some, 0)
        sums = jnp.concatenate([s_ref[at] for at in range(4)], axis=1)
        part_ref[zc] = dot3(halves(sums), (f_ref[0], f_ref[1]), dot_t)

    def half_of(ref, u):
        return ref.at[pl.ds(128 * u, 128)]

    def right_copy(h, u):
        src, dst = half_of(part_ref.at[(z + 4 - h) % 8], u), half_of(right_ref.at[h], u)
        return remote(src, dst, sendr.at[h, u], recvr.at[h, u], (slab, (z + 1) % 8, x))

    def left_copy(h, u):
        src, dst = half_of(part_ref.at[(z + 5 + h) % 8], u), half_of(left_ref.at[h], u)
        return remote(src, dst, sendl.at[h, u], recvl.at[h, u], (slab, (z + 7) % 8, x))

    def pass_on(zc, h, copy, held_ref):
        for u in range(2):
            rows = pl.ds(128 * u, 128)

            @pl.when(h > 0)
            def _():
                copy(jnp.maximum(h - 1, 0), u).wait_recv()
                part_ref[zc, rows, :] += held_ref[jnp.maximum(h - 1, 0), rows, :]

            copy(h, u).start()

    def outward(step, carry):
        h, odd = step // 2, step % 2
        zc = (z + (1 - odd) * (4 - h) + odd * (5 + h)) % 8
        collect(zc)

        @pl.when(odd == 0)
        def _():
            pass_on(zc, h, right_copy, right_ref)

        @pl.when((odd == 1) & (step < 7))
        def _():
            pass_on(zc, h, left_copy, left_ref)

        return carry

    fetch.wait()
    lax.fori_loop(0, 8, outward, 0)
    for u in range(2):
        left_copy(2, u).wait_recv()
        right_copy(3, u).wait_recv()
    total = part_ref[z] + (right_ref[3] + left_ref[2])
    sum_ref[...] = total

    def block(d):
        return pl.ds(pl.multiple_of(8 * d, 8), 8)

    def plane_copy(d):
        peer = (own + STEP32 * d) % 32
        return remote(sum_ref.at[block(peer)], tiles_ref.at[block(own)], sendp.at[d], recvp.at[own], place_of(peer, z))

    def plane_wait(d):
        peer = (own + STEP32 * d) % 32
        remote(sum_ref.at[block(peer)], tiles_ref.at[block(peer)], sendp.at[d], recvp.at[peer], place_of(peer, z)).wait_recv()

    each(32, lambda d: plane_copy(d).start())
    tiles_ref[block(own), :] = sum_ref[block(own), :]
    each(32, plane_wait)
    for u in range(2):
        for h in range(4):
            right_copy(h, u).wait_send()
            if h < 3:
                left_copy(h, u).wait_send()
    each(32, lambda d: plane_copy(d).wait_send())
    each(8, lambda d: word_copy(d).wait_send())
    each(32, lambda d: row_copy(d).wait_send())
    for c in range(CHUNKS):
        each(8, lambda d: slab_copy(c, d).wait_send())
        each(32, lambda d: row_block_copy(c, d).wait_send())

    tiles = jnp.concatenate([tiles_ref[pl.ds(k, 32, stride=8), :] for k in range(8)], axis=0)
    both = hdot(tiles, dr_ref[...])
    rows = []
    for k in range(8):
        cut = slice(32 * k, 32 * k + 32)
        y, iy = both[cut, 0:128], both[cut, 128:256]
        column = jnp.concatenate([jnp.concatenate([y, iy], axis=1), jnp.concatenate([iy, -y], axis=1)], axis=0)
        s_both = hdot(dl_ref[0], column)
        s, i_s = s_both[:, 0:128], s_both[:, 128:256]
        wa, wb = wa_ref[k], wb_ref[k]
        weighted = wa * s + wb * i_s
        found, i_found = [], []
        for half in range(2):
            at = k + 8 * half
            ar, ai = pa_ref[0, at], pa_ref[1, at]
            br, bi = pb_ref[0, at], pb_ref[1, at]
            phase = jnp.concatenate([jnp.concatenate([br, bi], axis=1), jnp.concatenate([-bi, br], axis=1)], axis=0)
            part = hdot(weighted[:, 64 * half : 64 * half + 64], phase)
            pr, pi = part[:, 0:128], part[:, 128:256]
            live = live_ref[pl.ds(at, 1), :]
            rr = (obs_ref[pl.ds(2 * at, 1), :] - jnp.sum(ar * pr - ai * pi, axis=0, keepdims=True)) * live
            ri = (obs_ref[pl.ds(2 * at + 1, 1), :] - jnp.sum(ar * pi + ai * pr, axis=0, keepdims=True)) * live
            vis_ref[pl.ds(2 * at, 1), :] = rr
            vis_ref[pl.ds(2 * at + 1, 1), :] = ri
            sr, si = ar * rr + ai * ri, ar * ri - ai * rr
            sent = jnp.concatenate([jnp.concatenate([sr, si], axis=1), jnp.concatenate([-si, sr], axis=1)], axis=0)
            back = hdot_t(sent, phase)
            found.append(back[0:32])
            i_found.append(back[32:64])
        c, ic = jnp.concatenate(found, axis=1), jnp.concatenate(i_found, axis=1)
        r, ir = wa * c - wb * ic, wa * ic + wb * c
        rows.append(hdot(dl_ref[1], jnp.concatenate([r, ir], axis=0)))
    tile = hdot_t(jnp.concatenate(rows, axis=0), dr_ref[:, 0:128])
    for k in range(8):
        back_ref[pl.ds(k, 32, stride=8), :] = tile[32 * k : 32 * k + 32]

    def block(d):
        return pl.ds(pl.multiple_of(8 * d, 8), 8)

    def plane_copy(d):
        peer = (own + STEP32 * d) % 32
        return remote(back_ref.at[block(peer)], g_ref.at[z, block(own)], sendq.at[d], recvq.at[own], place_of(peer, z))

    def plane_wait(d):
        peer = (own + STEP32 * d) % 32
        remote(back_ref.at[block(peer)], g_ref.at[z, block(peer)], sendq.at[d], recvq.at[peer], place_of(peer, z)).wait_recv()

    each(32, lambda d: plane_copy(d).start())
    g_ref[z, block(own), :] = back_ref[block(own), :]

    def quarter_wait(u):
        def one(step, carry):
            peer = 8 * u + step

            @pl.when(peer != own)
            def _():
                ref = g_ref.at[z, block(peer)]
                remote(ref, ref, sendq.at[0], recvq.at[peer], place_of((own + 1) % 32, z)).wait_recv()

            return carry

        lax.fori_loop(0, 8, one, 0)

    def right_copy(h, u):
        ref = g_ref.at[(z + 8 - h) % 8, pl.ds(64 * u, 64)]
        return remote(ref, ref, sendt.at[h, u], recvt.at[h, u], (slab, (z + 1) % 8, x))

    def left_copy(h, u):
        ref = g_ref.at[(z + h) % 8, pl.ds(64 * u, 64)]
        return remote(ref, ref, sendu.at[h, u], recvu.at[h, u], (slab, (z + 7) % 8, x))

    def right_wait(h, u):
        ref = g_ref.at[(z + 7 - h) % 8, pl.ds(64 * u, 64)]
        remote(ref, ref, sendt.at[h, u], recvt.at[h, u], (slab, (z + 1) % 8, x)).wait_recv()

    def left_wait(h, u):
        ref = g_ref.at[(z + 1 + h) % 8, pl.ds(64 * u, 64)]
        remote(ref, ref, sendu.at[h, u], recvu.at[h, u], (slab, (z + 7) % 8, x)).wait_recv()

    for h in range(4):
        for u in range(4):
            if h:
                right_wait(h - 1, u)
            else:
                quarter_wait(u)
            right_copy(h, u).start()
            if h < 3:
                if h:
                    left_wait(h - 1, u)
                left_copy(h, u).start()
    for u in range(4):
        left_wait(2, u)
        right_wait(3, u)
    each(32, lambda d: plane_copy(d).wait_send())
    for u in range(4):
        for h in range(4):
            right_copy(h, u).wait_send()
            if h < 3:
                left_copy(h, u).wait_send()


def scatter_kernel(
    idx_ref, tw_ref, f_ref, c_any, m_any, m1_any, w4_any, out_ref,
    w_ref, full_ref, l_ref, crep_ref, z0_ref, z1_ref, c_ref, m_ref, m1_ref, w4_ref, table,
):
    tables = [
        pltpu.make_async_copy(src, dst, table.at[at])
        for at, (src, dst) in enumerate(((w4_any, w4_ref), (m1_any, m1_ref), (c_any, c_ref), (m_any, m_ref)))
    ]
    for copy in tables:
        copy.start()

    def clear(step, carry):
        spots = pl.ds(pl.multiple_of(step * 128, 128), 128)
        zero = jnp.zeros((2, 128, 8, 128), F32)
        z0_ref[:, spots] = zero
        z1_ref[:, spots] = zero
        return carry

    lax.fori_loop(0, 16, clear, 0)
    for copy in tables:
        copy.wait()
    spread_screens(w4_ref, w_ref)
    fill_columns(m1_ref, full_ref)
    spread = dot3(halves(c_ref[...]), (f_ref[0], f_ref[1]))
    for at in range(4):
        crep_ref[at] = spread[:, 128 * at : 128 * at + 128]

    w_rows = w_ref.reshape(4096, 128)
    sets = (z0_ref.reshape(32768, 128), z1_ref.reshape(32768, 128))

    def add(it, carry):
        for k in range(16):
            z_rows = sets[k % 2]
            half, row = k // 8, k % 8
            word = idx_ref[it % 32, 0, it // 32 * 16 + k]
            spot, turn_row = pl.multiple_of(word & 16383, 8), pl.multiple_of(word >> 14, 8)
            cr = jnp.broadcast_to(crep_ref[2 * half, pl.ds(it * 8 + row, 1), :], (8, 128))
            ci = jnp.broadcast_to(crep_ref[2 * half + 1, pl.ds(it * 8 + row, 1), :], (8, 128))
            wr, wi = w_rows[pl.ds(turn_row, 8), :], w_rows[pl.ds(turn_row + 8, 8), :]
            z_rows[pl.ds(spot, 8), :] += cr * wr + ci * wi
            z_rows[pl.ds(spot + 16384, 8), :] += ci * wr - cr * wi
        return carry

    lax.fori_loop(0, 256, add, 0)

    def stage(step, carry):
        res = None
        for block in range(8):
            lanes = slice(256 * block, 256 * block + 256)
            spots = [pl.ds(pl.multiple_of(t % 8 * 256 + step * 32, 32), 32) for t in (2 * block, 2 * block + 1)]
            parts = [(z0_ref[block // 4, at] + z1_ref[block // 4, at]).reshape(256, 128) for at in spots]
            left = halves(jnp.concatenate(parts, axis=1))
            part = dot3(left, (full_ref[0:256, lanes], full_ref[256:512, lanes]), dot_t)
            res = part if res is None else res + part
        rows = pl.ds(pl.multiple_of(step * 256, 256), 256)
        l_ref[0, rows, :], l_ref[1, rows, :] = res[:, 0:128], res[:, 128:256]
        return carry

    lax.fori_loop(0, 8, stage, 0)

    wide = []
    for at in range(2):
        wide += halves(jnp.concatenate([l_ref[at, pl.ds(b, 256, stride=8), :] for b in range(8)], axis=1))
    cos, sin = (m_ref[0], m_ref[1]), (m_ref[2], m_ref[3])
    twr = jnp.concatenate([tw_ref[0]] * 2, axis=1)
    twi = jnp.concatenate([tw_ref[1]] * 2, axis=1)
    for x in range(4):
        place = placing(x)
        pieces = [dot_t(piece, place).astype(BF16) for piece in wide]
        ur, ui = (pieces[0], pieces[1]), (pieces[2], pieces[3])
        ar = dot3(cos, ur) - dot3(sin, ui)
        ai = dot3(cos, ui) + dot3(sin, ur)
        out_ref[:, x, 0] = (ar * twr + ai * twi).reshape(8, 32, 256)
        out_ref[:, x, 1] = (ai * twr - ar * twi).reshape(8, 32, 256)


def hdot(left, right):
    return jnp.dot(left, right, preferred_element_type=F32, precision=HIGHEST)


def hdot_t(left, right):
    return lax.dot_general(left, right, (((1,), (1,)), ((), ())), preferred_element_type=F32, precision=HIGHEST)


def subgrid_tables():
    index = np.arange(SUB)
    cos, sin = unit(index[:, None] * (index[None, :] - SUB // 2), SUB)
    one = np.block([[cos, sin], [-sin, cos]])
    turned = np.block([[-sin, cos], [-cos, -sin]])
    zero = np.zeros_like(one)
    right = np.concatenate([np.block([[one, zero], [zero, one]]), np.block([[turned, zero], [zero, turned]])], axis=1)
    left = np.stack([np.concatenate([cos.T, sin.T], axis=1), np.concatenate([cos, -sin], axis=1)])
    return right.astype(np.float32), (left / (SUB * SUB)).astype(np.float32)


def in_vmem(count):
    return [pl.BlockSpec(memory_space=pltpu.VMEM)] * count


def call(kernel, out, specs, scratch=(), collective_id=None, out_specs=None, vmem=62):
    return pl.pallas_call(
        kernel,
        out_shape=out,
        in_specs=specs,
        out_specs=out_specs or jax.tree.map(lambda _: pl.BlockSpec(memory_space=pltpu.VMEM), out),
        scratch_shapes=list(scratch),
        compiler_params=pltpu.CompilerParams(
            vmem_limit_bytes=vmem * 1024 * 1024, collective_id=collective_id, has_side_effects=collective_id is not None
        ),
    )


def f32(*shape):
    return jax.ShapeDtypeStruct(shape, F32)


SMEM = pl.BlockSpec(memory_space=pltpu.SMEM)


def per_device(model_image, vis_coords, vis_observed, tile_slot, tile_group, w_plane, vis_count):
    rows, columns, screens = row_tables(), column_tables(), screen_tables()
    right, left = subgrid_tables()

    vis, every, _, words, tw, spread = call(
        forward_kernel,
        (
            f32(32, 128),
            f32(8, 256, 128),
            jax.ShapeDtypeStruct((32, 1, 128), jnp.int32),
            jax.ShapeDtypeStruct((32, 1, 128), jnp.int32),
            f32(2, 256, 128),
            jax.ShapeDtypeStruct((2, 128, 512), BF16),
        ),
        [SMEM] * 4 + [ANY] + in_vmem(4) + [ANY] * 3,
        [
            pltpu.VMEM((2, 16, 32, 128), F32),
            pltpu.VMEM((2, 16, 32, 128), F32),
            pltpu.VMEM((8, 32, 128), F32),
            pltpu.VMEM((8, 32, 128), F32),
            pltpu.VMEM((16, 128), F32),
            pltpu.VMEM((256, 128), F32),
            pltpu.VMEM((256, 128), F32),
            pltpu.VMEM((1, 128), jnp.int32),
            pltpu.VMEM((8, 2, 4, 32, 256), F32),
            pltpu.VMEM((32, 2, 32, 256), F32),
            pltpu.VMEM((8, 1, 128), jnp.int32),
            pltpu.VMEM((1, 128), jnp.int32),
            pltpu.VMEM((32, 2, 32, 256), F32),
            pltpu.SMEM((32, 1, 128), jnp.int32),
            pltpu.VMEM((256, 2, 8, 128), F32),
            pltpu.VMEM((768, 2048), BF16),
            pltpu.VMEM((2, 2048, 128), F32),
            pltpu.VMEM((2, 2048, 128), F32),
            pltpu.VMEM((2, 2048, 8, 128), F32),
            pltpu.VMEM((4, 256, 128), F32),
            pltpu.VMEM((8, 256, 128), F32),
            pltpu.VMEM((4, 256, 128), F32),
            pltpu.VMEM((3, 256, 128), F32),
            pltpu.VMEM((256, 128), F32),
            DMA,
            DMA,
            DMA((CHUNKS, 8)),
            DMA((CHUNKS, 8)),
            DMA((CHUNKS, 32)),
            DMA((CHUNKS, 32)),
            DMA((8,)),
            DMA((8,)),
            DMA((32,)),
            DMA((32,)),
            DMA((4, 2)),
            DMA((4, 2)),
            DMA((3, 2)),
            DMA((3, 2)),
            DMA((32,)),
            DMA((32,)),
            DMA((32,)),
            DMA((32,)),
            DMA((4, 4)),
            DMA((4, 4)),
            DMA((3, 4)),
            DMA((3, 4)),
            pltpu.VMEM((4, 256, 256), BF16),
            pltpu.VMEM((4, 128, 1024), BF16),
            pltpu.VMEM((64, 2, 8, 128), F32),
            DMA((3,)),
        ],
        collective_id=0,
    )(
        tile_slot, tile_group[:, 0], w_plane, vis_count, model_image.reshape(2, 4, 8, 32, 256),
        vis_coords.reshape(32, 128), vis_observed.reshape(32, 128), right, left, rows, columns, screens,
    )
    every = every.reshape(2048, 128)
    spots = call(
        scatter_kernel,
        f32(8, 4, 2, 32, 256),
        [SMEM] + in_vmem(2) + [ANY] * 4,
        [
            pltpu.VMEM((256, 2, 8, 128), F32),
            pltpu.VMEM((768, 2048), BF16),
            pltpu.VMEM((2, 2048, 128), F32),
            pltpu.VMEM((4, 2048, 128), F32),
            pltpu.VMEM((2, 2048, 8, 128), F32),
            pltpu.VMEM((2, 2048, 8, 128), F32),
            pltpu.VMEM((2048, 128), F32),
            pltpu.VMEM((4, 256, 256), BF16),
            pltpu.VMEM((4, 128, 1024), BF16),
            pltpu.VMEM((64, 2, 8, 128), F32),
            DMA((4,)),
        ],
    )(words, tw, spread, every, rows, columns, screens)
    image = call(
        backward_kernel,
        f32(8, 2, 4, 32, 256),
        [HBM],
        [
            pltpu.VMEM((32, 2, 32, 256), F32),
            pltpu.VMEM((8, 2, 4, 32, 256), F32),
            DMA,
            DMA((CHUNKS,)),
            DMA((CHUNKS, 32)),
            DMA((CHUNKS, 32)),
            DMA((CHUNKS, 8)),
            DMA((CHUNKS, 8)),
        ],
        collective_id=2,
        out_specs=ANY,
        vmem=16,
    )(spots.reshape(32, 2, 32, 256))
    image = image.transpose(1, 2, 0, 3, 4).reshape(2, 1024, 256)
    return image, vis.reshape(16, 2, 128)


def solution(mesh):
    torus = Mesh(mesh.devices.reshape(mesh.shape["slab"], 8, 4), SLAB_BL)
    in_specs = (
        P(None, "slab", BL),
        P(SLAB_BL, None, None),
        P(SLAB_BL, None, None),
        P(SLAB_BL),
        P(SLAB_BL, None),
        P(SLAB_BL),
        P(SLAB_BL),
    )
    out_specs = (P(None, "slab", BL), P(SLAB_BL, None, None))
    return jax.shard_map(per_device, mesh=torus, in_specs=in_specs, out_specs=out_specs, check_vma=False)
```
